32 devices in a mesh: dp: 1 (over z), sp: 4 (over y), beam: 8 (over x, core).
Axes of the slice: x: 4, y: 4, z: 1, core: 2. Of those that a mesh axis runs over, the one named last changes fastest.
The devices are a block of a 4x4x8 slice.
Arguments:
- tok_emb: bfloat16 [48, 512], P(('dp', 'beam'))
- parent: int32 [2, 24], P('dp')
- position: int32 [1], replicated
- beam_score: float32 [48], P(('dp', 'beam'))
- k_cache: bfloat16 [2, 48, 1024, 8, 64], P(None, ('dp', 'beam'), 'sp')
- v_cache: bfloat16 [2, 48, 1024, 8, 64], P(None, ('dp', 'beam'), 'sp')
- w_query: bfloat16 [2, 512, 512], replicated
- w_key: bfloat16 [2, 512, 512], replicated
- w_value: bfloat16 [2, 512, 512], replicated
- w_out: bfloat16 [2, 512, 512], replicated
- w_gate: bfloat16 [2, 512, 2048], replicated
- w_up: bfloat16 [2, 512, 2048], replicated
- w_down: bfloat16 [2, 2048, 512], replicated
- g_attn: bfloat16 [2, 512], replicated
- g_mlp: bfloat16 [2, 512], replicated
- g_final: bfloat16 [512], replicated
- w_vocab: bfloat16 [512, 32128], replicated
Outputs:
- output 1: bfloat16 [2, 48, 1024, 8, 64], P(None, ('dp', 'beam'), 'sp')
- output 2: bfloat16 [2, 48, 1024, 8, 64], P(None, ('dp', 'beam'), 'sp')
- output 3: float32 [48, 32128], P(('dp', 'beam'))
All inputs are finite; a program needn't handle non-finite values.
Results may differ from the reference program's by a relative error of at most 0.00207768.
Values are sent between devices in bfloat16 or wider.
A program may use at most 768 MiB of HBM per device.

```python
import jax
import jax.numpy as jnp
from jax import lax

D_MODEL = 512
HEADS = 8
KV_HEADS = 8
HEAD = 64
FF = 2048
VOCAB = 32128
LAYERS = 2
WIDTH = 24
BEAMS = 48
SENTENCES = 2
SLOTS = 1024

ROPE_BASE = 10000.0
NORM_EPS = 1e-6


def scaled_normal(key_in, shape, fan_in):
    return (jax.random.normal(key_in, shape, jnp.float32) * fan_in ** -0.5).astype(jnp.bfloat16)


def setup_inputs(seed: int = 0, part: int = 0) -> dict:
    base_key = jax.random.key(seed)
    shared = jax.random.split(base_key, 16)
    part_keys = jax.random.split(jax.random.fold_in(base_key, part), 16)
    position = jax.random.randint(shared[0], (1,), SLOTS // 2, SLOTS, dtype=jnp.int32)
    dominant = jnp.repeat(jax.random.randint(part_keys[0], (SENTENCES,), 0, WIDTH, dtype=jnp.int32), WIDTH)
    coin_flip = jax.random.randint(part_keys[1], (BEAMS,), 0, 2, dtype=jnp.int32)
    anyone = jax.random.randint(part_keys[2], (BEAMS,), 0, WIDTH, dtype=jnp.int32)
    first_beam = (jnp.arange(BEAMS, dtype=jnp.int32) // WIDTH) * WIDTH
    parent = (first_beam + jnp.where(coin_flip == 1, dominant, anyone)).reshape(SENTENCES, WIDTH)
    tok_emb = jax.random.normal(part_keys[3], (BEAMS, D_MODEL), jnp.float32).astype(jnp.bfloat16)
    beam_score = -6.0 * jax.random.uniform(part_keys[4], (BEAMS,), jnp.float32)
    late_slot = (jnp.arange(SLOTS) > position[0]).astype(jnp.float32)
    slot_amp = jax.random.normal(part_keys[5], (LAYERS, BEAMS, SLOTS), jnp.float32) + 2.0 * late_slot
    amp_b = slot_amp[:, :, :, None, None]
    key_dir = jax.random.normal(part_keys[6], (LAYERS, BEAMS, 1, KV_HEADS, HEAD), jnp.float32)
    val_dir = jax.random.normal(part_keys[7], (LAYERS, BEAMS, 1, KV_HEADS, HEAD), jnp.float32)
    cache_shape = (LAYERS, BEAMS, SLOTS, KV_HEADS, HEAD)
    k_cache = (1.5 * amp_b * key_dir + 0.5 * jax.random.normal(part_keys[8], cache_shape, jnp.float32)).astype(jnp.bfloat16)
    v_cache = (amp_b * val_dir + 0.5 * jax.random.normal(part_keys[9], cache_shape, jnp.float32)).astype(jnp.bfloat16)
    return {
        'tok_emb': tok_emb,
        'parent': parent,
        'position': position,
        'beam_score': beam_score,
        'k_cache': k_cache,
        'v_cache': v_cache,
        'w_query': scaled_normal(shared[1], (LAYERS, D_MODEL, HEADS * HEAD), D_MODEL),
        'w_key': scaled_normal(shared[2], (LAYERS, D_MODEL, KV_HEADS * HEAD), D_MODEL),
        'w_value': scaled_normal(shared[3], (LAYERS, D_MODEL, KV_HEADS * HEAD), D_MODEL),
        'w_out': scaled_normal(shared[4], (LAYERS, HEADS * HEAD, D_MODEL), HEADS * HEAD),
        'w_gate': scaled_normal(shared[5], (LAYERS, D_MODEL, FF), D_MODEL),
        'w_up': scaled_normal(shared[6], (LAYERS, D_MODEL, FF), D_MODEL),
        'w_down': scaled_normal(shared[7], (LAYERS, FF, D_MODEL), FF),
        'g_attn': jax.random.uniform(shared[8], (LAYERS, D_MODEL), jnp.float32, 0.5, 1.5).astype(jnp.bfloat16),
        'g_mlp': jax.random.uniform(shared[9], (LAYERS, D_MODEL), jnp.float32, 0.5, 1.5).astype(jnp.bfloat16),
        'g_final': jax.random.uniform(shared[10], (D_MODEL,), jnp.float32, 0.5, 1.5).astype(jnp.bfloat16),
        'w_vocab': (jax.random.normal(shared[11], (D_MODEL, VOCAB), jnp.float32) * 2.0 * D_MODEL ** -0.5).astype(jnp.bfloat16),
    }


def rms_norm(x_in, g_vec):
    mean_sq = jnp.mean(x_in * x_in, axis=-1, keepdims=True)
    return (x_in * lax.rsqrt(mean_sq + NORM_EPS) * g_vec.astype(jnp.float32)).astype(jnp.bfloat16)


def rope_at(x_in, cur_pos):
    half_dim = x_in.shape[-1] // 2
    inv_freq = ROPE_BASE ** (-2.0 * jnp.arange(half_dim, dtype=jnp.float32) / x_in.shape[-1])
    angles = cur_pos.astype(jnp.float32) * inv_freq
    cos_t = jnp.cos(angles)
    sin_t = jnp.sin(angles)
    x_f = x_in.astype(jnp.float32)
    x_lo = x_f[..., :half_dim]
    x_hi = x_f[..., half_dim:]
    rotated = jnp.concatenate([x_lo * cos_t - x_hi * sin_t, x_hi * cos_t + x_lo * sin_t], axis=-1)
    return rotated.astype(jnp.bfloat16)


def reference(tok_emb, parent, position, beam_score, k_cache, v_cache, w_query, w_key, w_value, w_out, w_gate, w_up, w_down, g_attn, g_mlp, g_final, w_vocab):
    cur_pos = position[0]
    q_groups = HEADS // KV_HEADS
    att_scale = HEAD ** -0.5
    flat_parent = parent.reshape(BEAMS)
    slot_valid = jnp.arange(SLOTS) <= cur_pos
    k_moved = jnp.take(k_cache, flat_parent, axis=1)
    v_moved = jnp.take(v_cache, flat_parent, axis=1)

    def layer_fn(residual, layer_in):
        k_lay, v_lay, wq_l, wk_l, wv_l, wo_l, wg_l, wu_l, wd_l, ga_l, gm_l = layer_in
        hidden = rms_norm(residual, ga_l)
        queries = rope_at(jnp.dot(hidden, wq_l, preferred_element_type=jnp.float32).astype(jnp.bfloat16).reshape(BEAMS, HEADS, HEAD), cur_pos)
        key_new = rope_at(jnp.dot(hidden, wk_l, preferred_element_type=jnp.float32).astype(jnp.bfloat16).reshape(BEAMS, 1, KV_HEADS, HEAD), cur_pos)
        val_new = jnp.dot(hidden, wv_l, preferred_element_type=jnp.float32).astype(jnp.bfloat16).reshape(BEAMS, 1, KV_HEADS, HEAD)
        k_lay = lax.dynamic_update_slice_in_dim(k_lay, key_new, cur_pos, axis=1)
        v_lay = lax.dynamic_update_slice_in_dim(v_lay, val_new, cur_pos, axis=1)
        q_grp = queries.reshape(BEAMS, KV_HEADS, q_groups, HEAD)
        scores = jnp.einsum('bkgd,bskd->bkgs', q_grp.astype(jnp.float32), k_lay.astype(jnp.float32)) * att_scale
        scores = jnp.where(slot_valid, scores, -jnp.inf)
        row_max = jnp.max(scores, axis=-1, keepdims=True)
        exp_scores = jnp.exp(scores - row_max)
        exp_total = jnp.sum(exp_scores, axis=-1)
        mix_sum = jnp.einsum('bkgs,bskd->bkgd', exp_scores.astype(jnp.bfloat16).astype(jnp.float32), v_lay.astype(jnp.float32))
        attn_out = (mix_sum / exp_total[..., None]).astype(jnp.bfloat16).reshape(BEAMS, HEADS * HEAD)
        residual = residual + jnp.dot(attn_out, wo_l, preferred_element_type=jnp.float32).astype(jnp.bfloat16).astype(jnp.float32)
        hidden = rms_norm(residual, gm_l)
        gate_act = jnp.dot(hidden, wg_l, preferred_element_type=jnp.float32).astype(jnp.bfloat16)
        up_act = jnp.dot(hidden, wu_l, preferred_element_type=jnp.float32).astype(jnp.bfloat16)
        swi_out = (jax.nn.silu(gate_act.astype(jnp.float32)) * up_act.astype(jnp.float32)).astype(jnp.bfloat16)
        residual = residual + jnp.dot(swi_out, wd_l, preferred_element_type=jnp.float32).astype(jnp.bfloat16).astype(jnp.float32)
        return residual, (k_lay, v_lay)

    layer_inputs = (k_moved, v_moved, w_query, w_key, w_value, w_out, w_gate, w_up, w_down, g_attn, g_mlp)
    residual, layer_caches = lax.scan(layer_fn, tok_emb.astype(jnp.float32), layer_inputs)
    k_out, v_out = layer_caches
    hidden = rms_norm(residual, g_final)
    logits = jnp.dot(hidden, w_vocab, preferred_element_type=jnp.float32)
    candidates = jnp.take(beam_score, flat_parent)[:, None] + jax.nn.log_softmax(logits, axis=-1)
    return (k_out, v_out, candidates)
```

```python
import functools

import jax
import jax.numpy as jnp
from jax import lax
from jax.experimental import pallas as pl
from jax.experimental.pallas import tpu as pltpu
from jax.sharding import PartitionSpec as P

ROPE_BASE = 10000.0
NORM_EPS = 1e-6
NEG = -1e30
CORES = 2
LEVELS = (12,)
CHUNK = 2048
VBUF = 4
VMEM_LIMIT = 64 * 1024 * 1024 - 64 * 1024
MESH = pl.DeviceIdType.MESH
F32 = jnp.float32
BF16 = jnp.bfloat16


def rms(x, g):
    ms = jnp.mean(x * x, axis=-1, keepdims=True)
    return (x * lax.rsqrt(ms + NORM_EPS) * g.astype(F32)).astype(BF16)


def plan_kernel(dims, parent_ref, score_ref, tok_ref, plan_ref, pay_ref, pm_ref, rank_ref):
    nb, span = dims
    rows = CORES * nb
    n_sent, width = parent_ref.shape
    me = lax.axis_index('beam')
    sent = me // span
    place = lax.rem(me, span)
    chip = lax.div(place, CORES)

    def needed(s, to_chip):
        base = (1 - to_chip) * rows
        mask = jnp.int32(0)
        for k in range(rows):
            p = parent_ref[s, to_chip * rows + k] - s * width - base
            mask = mask | jnp.where((p >= 0) & (p < rows), jnp.left_shift(jnp.int32(1), jnp.clip(p, 0, rows - 1)), 0)
        return mask

    def bit(mask, p):
        return jnp.right_shift(mask, p) & 1

    most = jnp.int32(0)
    for s in range(n_sent):
        for tc in range(2):
            m = needed(s, tc)
            most = jnp.maximum(most, sum(bit(m, p) for p in range(rows)))
    out_mask = needed(sent, 1 - chip)
    in_mask = needed(sent, chip)
    for p in range(rows + 1):
        plan_ref[p] = 0
    cnt = jnp.int32(0)
    for p in range(rows):
        @pl.when(bit(out_mask, p) == 1)
        def _(p=p, cnt=cnt):
            plan_ref[cnt] = p
        cnt = cnt + bit(out_mask, p)
    cnt = jnp.int32(0)
    for p in range(rows):
        rank_ref[p] = cnt
        cnt = cnt + bit(in_mask, p)
    for b in range(nb):
        par = parent_ref[sent, place * nb + b] - sent * width
        dev = lax.div(par, nb)
        row = lax.rem(par, nb)
        far = lax.div(dev, CORES) != chip
        slot = rank_ref[jnp.clip(par - (1 - chip) * rows, 0, rows - 1)]
        plan_ref[rows + b] = jnp.where(far, 2, jnp.where(dev == place, 0, 1))
        plan_ref[rows + nb + b] = jnp.where(far, slot, row)
    plan_ref[rows + 2 * nb] = most
    for i in range(span):
        for b in range(8):
            if b < nb:
                par = parent_ref[sent, i * nb + b] - sent * width
                code = lax.div(par, nb) * 8 + lax.rem(par, nb)
            else:
                code = jnp.int32(-1)
            pm_ref[i * 8 + b:i * 8 + b + 1, :] = jnp.full((1, pm_ref.shape[1]), code, jnp.int32)
    lane = lax.broadcasted_iota(jnp.int32, (1, pay_ref.shape[1]), 1)
    row = jnp.zeros((1, pay_ref.shape[1]), F32)
    for b in range(nb):
        row = jnp.where(lane == b, score_ref[b], row)
    pay_ref[0:nb, :] = tok_ref[...].astype(F32)
    pay_ref[nb:nb + 1, :] = row
    pay_ref[nb + 1:8, :] = jnp.zeros((8 - nb - 1, pay_ref.shape[1]), F32)


def main_kernel(dims, n_slots, plan_ref, pos_ref, pay_ref, pm_ref, cs_ref, ga_ref, gm_ref, gf_ref,
                k_ref, v_ref, wq_ref, wk_ref, wv_ref, wo_ref, wg_ref, wu_ref, wd_ref, wvoc_ref,
                cand_ref, new_ref, sib_ref, recv_ref,
                pk0, pk1, pk2, pk3, stage, kv_att, b_q, b_k, b_v, b_o, b_g, b_u, b_d, vbuf,
                payall, resid, qbuf, knew, vnew, pbuf, rbuf, abuf, gbuf, attn,
                s_pl, s_pr, s_pkl, s_pks, s_pkr, s_sib, s_ss, s_sr, s_bs, s_br, s_fs, s_fr,
                s_att, s_w, s_voc, s_1s, s_1r, s_2s, s_2r):
    nb, span, sp_n, hd = dims
    n_layers = ga_ref.shape[0]
    dm = ga_ref.shape[1]
    slots = k_ref.shape[3]
    half = k_ref.shape[2] // 2
    seq = lax.axis_index('sp')
    me = lax.axis_index('beam')
    place = lax.rem(me, span)
    base = me - place
    core = lax.rem(me, CORES)
    other = 1 - core
    rows = CORES * nb
    sib = {'beam': base + lax.div(place, CORES) * CORES + other}
    par = {'beam': base + lax.rem(place + CORES, span)}

    def peer(di, dj):
        return {'beam': base + lax.rem(place + di, span), 'sp': lax.rem(seq + dj, sp_n)}

    everyone = [(di, dj) for di in range(span) for dj in range(sp_n) if (di, dj) != (0, 0)]

    barrier = pltpu.get_barrier_semaphore()
    for di, dj in everyone:
        pl.semaphore_signal(barrier, inc=1, device_id=peer(di, dj), device_id_type=MESH)

    def local(src, dst, sem):
        c = pltpu.make_async_copy(src, dst, sem)
        c.start()
        return c

    def remote(src, dst, ss, rs, dev):
        return pltpu.make_async_remote_copy(src_ref=src, dst_ref=dst, send_sem=ss, recv_sem=rs,
                                            device_id=dev, device_id_type=MESH)

    pks = (pk0, pk1, pk2, pk3)
    chunks = [(src, pl.ds(h * half, half)) for src in (k_ref, v_ref) for h in range(2)]
    pk_local = [local(src.at[core, :, hs], pks[i].at[pl.ds(core * nb, nb)], s_pkl.at[i])
                for i, (src, hs) in enumerate(chunks)]
    w0 = [local(src.at[0], dst.at[0], s_w.at[0, i])
          for i, (src, dst) in enumerate(((wq_ref, b_q), (wk_ref, b_k), (wv_ref, b_v)))]
    att = {}
    for l in range(n_layers):
        for i, src in enumerate((k_ref, v_ref)):
            att[l, i] = local(src.at[l], kv_att.at[l, i], s_att.at[l, i])
    weights = {}
    pairs = ((wq_ref, b_q), (wk_ref, b_k), (wv_ref, b_v), (wo_ref, b_o), (wg_ref, b_g), (wu_ref, b_u), (wd_ref, b_d))
    for l in range(n_layers):
        for i, (src, dst) in enumerate(pairs):
            weights[l, i] = w0[i] if (l == 0 and i < 3) else local(src.at[l], dst.at[l], s_w.at[l, i])
    vocab = wvoc_ref.shape[1]
    n_full = vocab // CHUNK
    tail = vocab - n_full * CHUNK

    def voc_copy(i, slot):
        return pltpu.make_async_copy(wvoc_ref.at[:, pl.ds(i * CHUNK, CHUNK)], vbuf.at[slot], s_voc.at[slot])

    def voc_tail():
        return pltpu.make_async_copy(wvoc_ref.at[:, pl.ds(n_full * CHUNK, tail)],
                                     vbuf.at[n_full % VBUF, :, pl.ds(0, tail)], s_voc.at[n_full % VBUF])

    for i in range(VBUF):
        voc_copy(i, i).start()

    pl.semaphore_wait(barrier, len(everyone))

    pay_out = []
    for di in range(1, span):
        c = remote(pay_ref, payall.at[di], s_pl.at[di], s_pr.at[di], peer(di, 0))
        c.start()
        pay_out.append(c)
    sib_pk = []
    for i, (src, hs) in enumerate(chunks):
        c = remote(src.at[other, :, hs], pks[i].at[pl.ds(core * nb, nb)], s_pks.at[i], s_pkr.at[i], sib)
        c.start()
        sib_pk.append(c)
    sib_rest = []
    for i, src in enumerate((k_ref, v_ref)):
        c = remote(src.at[core], sib_ref.at[core, i], s_ss.at[i], s_sr.at[i], sib)
        c.start()
        sib_rest.append(c)

    def bulk(ch, s):
        dst = recv_ref.at[core, ch // 2, s, pl.ds((ch % 2) * half, half)]
        return remote(stage.at[ch, s], dst, s_bs.at[ch, s], s_br.at[ch, s], par)

    def forward(ch, s):
        ref = recv_ref.at[core, ch // 2, s, pl.ds((ch % 2) * half, half)]
        return remote(ref, ref, s_fs.at[ch, s], s_fr.at[ch, s], sib)

    sib_home = []

    def pack(ch):
        pk_local[ch].wait()
        sib_pk[ch].wait_recv()
        for s in range(n_slots):
            stage[ch, s] = pks[ch][plan_ref[s]]
        hs = pl.ds((ch % 2) * half, half)
        sib_home.append(local(pks[ch].at[pl.ds(other * nb, nb)], sib_ref.at[core, ch // 2, :, hs], s_sib.at[ch]))

    units = [(ch, s) for ch in range(4) for s in range(n_slots)]
    issued = [0]

    def issue(count):
        for ch, s in units[issued[0]:issued[0] + count]:
            bulk(ch, s).start()
        issued[0] = min(len(units), issued[0] + count)

    pack(0)
    issue(min(3, n_slots))

    payall[0] = pay_ref[...]
    for c in pay_out:
        c.wait_recv()
    for i in range(span):
        resid[pl.ds(pl.multiple_of(i * 8, 8), 8), :] = payall[lax.rem(place - i + span, span)]

    lane = lax.broadcasted_iota(jnp.int32, (1, dm), 1)
    low = lax.rem(lane, hd) < hd // 2
    t = pos_ref[0]
    att_scale = hd ** -0.5
    cosv = cs_ref[0:1, :]
    sinv = cs_ref[1:2, :]

    def rope(x):
        swapped = jnp.where(low, pltpu.roll(x, dm - hd // 2, 1), pltpu.roll(x, hd // 2, 1))
        return x * cosv + swapped * sinv

    qw = 256
    hq = qw // hd
    n_quad = dm // qw
    lane_q = lax.broadcasted_iota(jnp.int32, (1, qw), 1)
    head_mask = [lax.div(lane_q, hd) == h for h in range(hq)]
    slot_id = seq * slots + lax.broadcasted_iota(jnp.int32, (1, slots), 1)
    valid = slot_id < t
    pm = pm_ref[...]
    pm4 = jnp.concatenate([pm] * hq, axis=0)
    nrow = pm.shape[0]

    for l in range(n_layers):
        hidden = rms(resid[...], ga_ref[l:l + 1, :])
        for i in range(3):
            weights[l, i].wait()
        q = jnp.dot(hidden, b_q[l], preferred_element_type=F32).astype(BF16).astype(F32)
        k = jnp.dot(hidden, b_k[l], preferred_element_type=F32).astype(BF16).astype(F32)
        v = jnp.dot(hidden, b_v[l], preferred_element_type=F32).astype(BF16).astype(F32)
        q = rope(q).astype(BF16).astype(F32)
        k = rope(k).astype(BF16).astype(F32)
        qbuf[...] = q
        knew[...] = k
        vnew[...] = v
        mine = pl.ds(pl.multiple_of(place * 8, 8), 8)
        new_ref[l, 0] = knew[mine, :]
        new_ref[l, 1] = vnew[mine, :]
        if l == 0:
            for ch in range(1, 4):
                pack(ch)
        att[l, 0].wait()
        att[l, 1].wait()
        for g in range(n_quad):
            gs = pl.ds(g * qw, qw)
            qg = q[:, g * qw:(g + 1) * qw]
            qq = jnp.concatenate([jnp.where(hm, qg, 0.0) for hm in head_mask], axis=0).astype(BF16)
            s = jnp.zeros((hq * nrow, slots), F32)
            for c in range(nb):
                sc = jnp.dot(qq, kv_att[l, 0, c, gs], preferred_element_type=F32)
                s = jnp.where(pm4 == place * 8 + c, sc, s)
            s = jnp.where(valid, s * att_scale, NEG)
            m = jnp.max(s, axis=-1, keepdims=True)
            e = jnp.where(valid, jnp.exp(s - m), 0.0)
            den = jnp.sum(e, axis=-1, keepdims=True)
            acc = jnp.zeros((hq * nrow, qw), F32)
            for c in range(nb):
                ec = jnp.where(pm4 == place * 8 + c, e, 0.0).astype(BF16)
                acc = acc + lax.dot_general(ec, kv_att[l, 1, c, gs], (((1,), (1,)), ((), ())),
                                            preferred_element_type=F32)

            def fold(x):
                y = jnp.zeros((nrow, qw), F32)
                for h in range(hq):
                    y = jnp.where(head_mask[h], x[h * nrow:(h + 1) * nrow], y)
                return y

            for j, x in enumerate((fold(acc), fold(m), fold(den))):
                for w in range(qw // 128):
                    pbuf[l, g * (qw // 128) + w, j] = x[:, w * 128:(w + 1) * 128]
        ex1 = []
        for dj in range(1, sp_n):
            c = remote(pbuf.at[l, lax.rem(seq + dj, sp_n)], rbuf.at[l, dj], s_1s.at[l, dj], s_1r.at[l, dj], peer(0, dj))
            c.start()
            ex1.append(c)
        rbuf[l, 0] = pbuf[l, seq]
        js = pl.ds(pl.multiple_of(seq * 128, 128), 128)
        prod = qbuf[:, js] * knew[:, js]
        lane2 = lax.broadcasted_iota(jnp.int32, (1, 128), 1)
        s_new = jnp.zeros((nrow, 128), F32)
        for h in range(128 // hd):
            hm = lax.div(lane2, hd) == h
            s_new = jnp.where(hm, jnp.sum(jnp.where(hm, prod, 0.0), axis=-1, keepdims=True), s_new)
        s_new = s_new * att_scale
        for c in ex1:
            c.wait_recv()
        m_all = s_new
        for dj in range(sp_n):
            m_all = jnp.maximum(m_all, rbuf[l, dj, 1])
        w_new = jnp.exp(s_new - m_all)
        num = w_new * vnew[:, js]
        den = w_new
        for dj in range(sp_n):
            wj = jnp.exp(rbuf[l, dj, 1] - m_all)
            num = num + wj * rbuf[l, dj, 0]
            den = den + wj * rbuf[l, dj, 2]
        o = jnp.where(lax.div(pm[:, 0:128], 8) == place, num / den, 0.0).astype(BF16)
        abuf[l] = o
        ex2 = []
        for n, (di, dj) in enumerate(everyone):
            c = remote(abuf.at[l], gbuf.at[l, n + 1], s_2s.at[l, n], s_2r.at[l, n], peer(di, dj))
            c.start()
            ex2.append(c)
        issue(4 if l == 0 else len(units))
        gbuf[l, 0] = o
        for i in range(3, 7):
            weights[l, i].wait()
        for c in ex2:
            c.wait_recv()
        for dj in range(sp_n):
            total = gbuf[l, dj].astype(F32)
            for di in range(1, span):
                total = total + gbuf[l, di * sp_n + dj].astype(F32)
            off = pl.multiple_of(lax.rem(seq - dj + sp_n, sp_n) * 128, 128)
            attn[:, pl.ds(off, 128)] = total
        r = resid[...]
        r = r + jnp.dot(attn[...].astype(BF16), b_o[l], preferred_element_type=F32).astype(BF16).astype(F32)
        hidden = rms(r, gm_ref[l:l + 1, :])
        gate = jnp.dot(hidden, b_g[l], preferred_element_type=F32).astype(BF16).astype(F32)
        up = jnp.dot(hidden, b_u[l], preferred_element_type=F32).astype(BF16).astype(F32)
        act = (gate * jax.nn.sigmoid(gate) * up).astype(BF16)
        r = r + jnp.dot(act, b_d[l], preferred_element_type=F32).astype(BF16).astype(F32)
        resid[...] = r
        for c in ex1 + ex2:
            c.wait_send()

    own = resid[pl.ds(pl.multiple_of(place * 8, 8), 8), :]
    hv = rms(own, gf_ref[...])

    @pl.loop(0, n_full)
    def _(i):
        slot = lax.rem(i, VBUF)
        voc_copy(i, slot).wait()
        cand_ref[:, pl.ds(pl.multiple_of(i * CHUNK, CHUNK), CHUNK)] = jnp.dot(
            hv, vbuf[slot], preferred_element_type=F32)

        @pl.when(i + VBUF < n_full)
        def _():
            voc_copy(i + VBUF, slot).start()

        if tail:
            @pl.when(i + VBUF == n_full)
            def _():
                voc_tail().start()

    if tail:
        voc_tail().wait()
        cand_ref[:, pl.ds(n_full * CHUNK, tail)] = jnp.dot(
            hv, vbuf[n_full % VBUF, :, pl.ds(0, tail)], preferred_element_type=F32)

    lg = cand_ref[...]
    mx = jnp.max(lg, axis=-1, keepdims=True)
    lse = jnp.log(jnp.sum(jnp.exp(lg - mx), axis=-1, keepdims=True))
    code = pm_ref[pl.ds(pl.multiple_of(place * 8, 8), 8), 0:128]
    lane1 = lax.broadcasted_iota(jnp.int32, (1, 128), 1)
    score = jnp.zeros((8, 1), F32)
    for i in range(span):
        dev = lax.rem(place - i + span, span)
        srow = payall[i, nb:nb + 1, 0:128]
        score = score + jnp.sum(jnp.where(code == dev * 8 + lane1, srow, 0.0), axis=-1, keepdims=True)
    cand_ref[...] = score + ((cand_ref[...] - mx) - lse)

    for ch in range(4):
        @pl.loop(0, n_slots)
        def _(s, ch=ch):
            bulk(ch, s).wait_recv()
            forward(ch, s).start()
    for c in pay_out + sib_pk + sib_rest:
        c.wait_send()
    for c in sib_rest:
        c.wait_recv()
    for c in sib_home:
        c.wait()
    for ch in range(4):
        @pl.loop(0, n_slots)
        def _(s, ch=ch):
            bulk(ch, s).wait_send()
            forward(ch, s).wait_send()
            ref = recv_ref.at[other, ch // 2, s, pl.ds((ch % 2) * half, half)]
            remote(ref, ref, s_fs.at[ch, s], s_fr.at[ch, s], sib).wait_recv()


def assemble_kernel(dims, plan_ref, pos_ref, new_ref, cand8_ref, k_ref, v_ref, sib_ref, recv_ref,
                    ko_ref, vo_ref, cand_ref, buf, s_in, s_out):
    nb = dims[0]
    rows = CORES * nb
    n_layers = k_ref.shape[0]
    slots = k_ref.shape[3]
    seq = lax.axis_index('sp')
    at = pos_ref[0] - seq * slots
    owns = (at >= 0) & (at < slots)
    order = [(l, i, b) for l in range(n_layers) for i in range(2) for b in range(nb)]
    for u, (l, i, b) in enumerate(order):
        kind = plan_ref[rows + b]
        idx = plan_ref[rows + nb + b]
        src = (k_ref, v_ref)[i]

        @pl.when(kind == 0)
        def _():
            pltpu.make_async_copy(src.at[l, idx], buf.at[u], s_in.at[u]).start()

        @pl.when(kind == 1)
        def _():
            pltpu.make_async_copy(sib_ref.at[l, i, idx], buf.at[u], s_in.at[u]).start()

        @pl.when(kind == 2)
        def _():
            pltpu.make_async_copy(recv_ref.at[l, i, idx], buf.at[u], s_in.at[u]).start()

    cand_ref[...] = cand8_ref[0:nb, :]
    tile = jnp.clip(lax.div(at, 128), 0, slots // 128 - 1)
    lane = lax.broadcasted_iota(jnp.int32, (1, 128), 1)
    outs = []
    for l in range(n_layers):
        for i in range(2):
            cols = jnp.transpose(new_ref[l, i])
            for b in range(nb):
                u = (l * 2 + i) * nb + b
                pltpu.make_async_copy((k_ref, v_ref)[i].at[l, b], buf.at[u], s_in.at[u]).wait()

                @pl.when(owns)
                def _():
                    ts = pl.ds(pl.multiple_of(tile * 128, 128), 128)
                    old = buf[u, :, ts]
                    buf[u, :, ts] = jnp.where(lane == at - tile * 128, cols[:, b:b + 1].astype(BF16), old)

                c = pltpu.make_async_copy(buf.at[u], (ko_ref, vo_ref)[i].at[l, b], s_out.at[u])
                c.start()
                outs.append(c)
    for c in outs:
        c.wait()


def solution(mesh):
    beam_spec = P(('dp', 'beam'))
    row_spec = P(('dp', 'beam'), None)
    cache_spec = P(None, ('dp', 'beam'), 'sp', None, None)
    rep = P()
    sp_n = mesh.shape['sp']

    def local_step(tok_emb, parent, position, beam_score, k_cache, v_cache, w_query, w_key, w_value, w_out,
                   w_gate, w_up, w_down, g_attn, g_mlp, g_final, w_vocab):
        n_layers, nb, slots, heads, hd = k_cache.shape
        width = parent.shape[1]
        span = width // nb
        dm = tok_emb.shape[1]
        ff = w_gate.shape[2]
        vocab = w_vocab.shape[1]
        rows = CORES * nb
        hrow = heads * hd
        kt = k_cache.transpose(0, 1, 3, 4, 2).reshape(n_layers, nb, hrow, slots)
        vt = v_cache.transpose(0, 1, 3, 4, 2).reshape(n_layers, nb, hrow, slots)
        smem = pl.BlockSpec(memory_space=pltpu.SMEM)
        vmem = pl.BlockSpec(memory_space=pltpu.VMEM)
        hbm = pl.BlockSpec(memory_space=pl.ANY)
        sds = jax.ShapeDtypeStruct

        plan, pay, pm = pl.pallas_call(
            functools.partial(plan_kernel, (nb, span)),
            out_shape=(sds((64,), jnp.int32), sds((8, dm), F32), sds((8 * span, slots), jnp.int32)),
            in_specs=[smem, smem, vmem], out_specs=(smem, vmem, vmem),
            scratch_shapes=[pltpu.SMEM((rows,), jnp.int32)],
            name='plan',
        )(parent, beam_score, tok_emb)

        half_dim = hd // 2
        inv_freq = ROPE_BASE ** (-2.0 * jnp.arange(half_dim, dtype=F32) / hd)
        angles = position[0].astype(F32) * inv_freq
        cos_t, sin_t = jnp.cos(angles), jnp.sin(angles)
        cs = jnp.stack([jnp.tile(jnp.concatenate([cos_t, cos_t]), heads),
                        jnp.tile(jnp.concatenate([-sin_t, sin_t]), heads)])

        def main(n_slots, cid, *ops):
            half = hrow // 2
            np_ = dm // 128
            nrow = 8 * span
            dma = pltpu.SemaphoreType.DMA
            scratch = [pltpu.VMEM((rows, half, slots), BF16)] * 4 + [
                pltpu.VMEM((4, n_slots, half, slots), BF16),
                pltpu.VMEM((n_layers, 2, nb, hrow, slots), BF16),
                pltpu.VMEM((n_layers, dm, hrow), BF16),
                pltpu.VMEM((n_layers, dm, hrow), BF16),
                pltpu.VMEM((n_layers, dm, hrow), BF16),
                pltpu.VMEM((n_layers, hrow, dm), BF16),
                pltpu.VMEM((n_layers, dm, ff), BF16),
                pltpu.VMEM((n_layers, dm, ff), BF16),
                pltpu.VMEM((n_layers, ff, dm), BF16),
                pltpu.VMEM((VBUF, dm, CHUNK), BF16),
                pltpu.VMEM((span, 8, dm), F32),
                pltpu.VMEM((nrow, dm), F32),
                pltpu.VMEM((nrow, dm), F32),
                pltpu.VMEM((nrow, dm), F32),
                pltpu.VMEM((nrow, dm), F32),
                pltpu.VMEM((n_layers, np_, 3, nrow, 128), F32),
                pltpu.VMEM((n_layers, sp_n, 3, nrow, 128), F32),
                pltpu.VMEM((n_layers, nrow, 128), BF16),
                pltpu.VMEM((n_layers, span * sp_n, nrow, 128), BF16),
                pltpu.VMEM((nrow, dm), F32),
                dma((span,)), dma((span,)),
                dma((4,)), dma((4,)), dma((4,)), dma((4,)), dma((2,)), dma((2,)),
                dma((4, n_slots)), dma((4, n_slots)), dma((4, n_slots)), dma((4, n_slots)),
                dma((n_layers, 2)), dma((n_layers, 7)), dma((VBUF,)),
                dma((n_layers, sp_n)), dma((n_layers, sp_n)),
                dma((n_layers, span * sp_n)), dma((n_layers, span * sp_n)),
            ]
            return pl.pallas_call(
                functools.partial(main_kernel, (nb, span, sp_n, hd), n_slots),
                out_shape=(sds((8, vocab), F32), sds((n_layers, 2, 8, hrow), F32),
                           sds((n_layers, 2, nb, hrow, slots), BF16),
                           sds((n_layers, 2, rows, hrow, slots), BF16)),
                in_specs=[smem, smem] + [vmem] * 6 + [hbm] * 10,
                out_specs=(vmem, vmem, hbm, hbm),
                scratch_shapes=scratch,
                compiler_params=pltpu.CompilerParams(collective_id=cid, has_side_effects=True,
                                                     vmem_limit_bytes=VMEM_LIMIT),
                name=f'main{n_slots}',
            )(*ops)

        ops = (plan, position, pay, pm, cs, g_attn, g_mlp, g_final.reshape(1, dm), kt, vt,
               w_query, w_key, w_value, w_out, w_gate, w_up, w_down, w_vocab)
        cand8, new, sib, recv = main(LEVELS[-1], 0, *ops)

        ko, vo, cand = pl.pallas_call(
            functools.partial(assemble_kernel, (nb,)),
            out_shape=(sds(kt.shape, BF16), sds(vt.shape, BF16), sds((nb, vocab), F32)),
            in_specs=[smem, smem, vmem, vmem, hbm, hbm, hbm, hbm],
            out_specs=(hbm, hbm, vmem),
            scratch_shapes=[pltpu.VMEM((n_layers * 2 * nb, hrow, slots), BF16),
                            pltpu.SemaphoreType.DMA((n_layers * 2 * nb,)),
                            pltpu.SemaphoreType.DMA((n_layers * 2 * nb,))],
            compiler_params=pltpu.CompilerParams(vmem_limit_bytes=VMEM_LIMIT),
            name='assemble',
        )(plan, position, new, cand8, kt, vt, sib, recv)

        def back(x):
            return x.reshape(n_layers, nb, heads, hd, slots).transpose(0, 1, 4, 2, 3)

        return back(ko), back(vo), cand

    in_specs = (row_spec, P('dp', None), rep, beam_spec, cache_spec, cache_spec) + (rep,) * 11
    return jax.shard_map(local_step, mesh=mesh, in_specs=in_specs, out_specs=(cache_spec, cache_spec, row_spec),
                         check_vma=False)
```

```python
import functools

import jax
import jax.numpy as jnp
from jax import lax
from jax.experimental import pallas as pl
from jax.experimental.pallas import tpu as pltpu
from jax.sharding import PartitionSpec as P

ROPE_BASE = 10000.0
NORM_EPS = 1e-6
NEG = -1e30
CORES = 2
LEVELS = (3, 4, 5, 6)
CHUNK = 2048
VBUF = 4
VMEM_LIMIT = 64 * 1024 * 1024 - 64 * 1024
MESH = pl.DeviceIdType.MESH
F32 = jnp.float32
BF16 = jnp.bfloat16


def rms(x, g):
    ms = jnp.mean(x * x, axis=-1, keepdims=True)
    return (x * lax.rsqrt(ms + NORM_EPS) * g.astype(F32)).astype(BF16)


def plan_kernel(dims, parent_ref, score_ref, tok_ref, plan_ref, pay_ref, pm_ref, rank_ref):
    nb, span = dims
    rows = CORES * nb
    n_sent, width = parent_ref.shape
    me = lax.axis_index('beam')
    sent = me // span
    place = lax.rem(me, span)
    chip = lax.div(place, CORES)

    def needed(s, to_chip):
        base = (1 - to_chip) * rows
        mask = jnp.int32(0)
        for k in range(rows):
            p = parent_ref[s, to_chip * rows + k] - s * width - base
            mask = mask | jnp.where((p >= 0) & (p < rows), jnp.left_shift(jnp.int32(1), jnp.clip(p, 0, rows - 1)), 0)
        return mask

    def bit(mask, p):
        return jnp.right_shift(mask, p) & 1

    most = jnp.int32(0)
    for s in range(n_sent):
        for tc in range(2):
            m = needed(s, tc)
            most = jnp.maximum(most, sum(bit(m, p) for p in range(rows)))
    out_mask = needed(sent, 1 - chip)
    in_mask = needed(sent, chip)
    for p in range(rows + 1):
        plan_ref[p] = 0
    cnt = jnp.int32(0)
    for p in range(rows):
        @pl.when(bit(out_mask, p) == 1)
        def _(p=p, cnt=cnt):
            plan_ref[cnt] = p
        cnt = cnt + bit(out_mask, p)
    cnt = jnp.int32(0)
    for p in range(rows):
        rank_ref[p] = cnt
        cnt = cnt + bit(in_mask, p)
    for b in range(nb):
        par = parent_ref[sent, place * nb + b] - sent * width
        dev = lax.div(par, nb)
        row = lax.rem(par, nb)
        far = lax.div(dev, CORES) != chip
        slot = rank_ref[jnp.clip(par - (1 - chip) * rows, 0, rows - 1)]
        plan_ref[rows + b] = jnp.where(far, 2, jnp.where(dev == place, 0, 1))
        plan_ref[rows + nb + b] = jnp.where(far, slot, row)
    plan_ref[rows + 2 * nb] = most
    for i in range(span):
        for b in range(8):
            if b < nb:
                par = parent_ref[sent, i * nb + b] - sent * width
                code = lax.div(par, nb) * 8 + lax.rem(par, nb)
            else:
                code = jnp.int32(-1)
            pm_ref[i * 8 + b:i * 8 + b + 1, :] = jnp.full((1, pm_ref.shape[1]), code, jnp.int32)
    lane = lax.broadcasted_iota(jnp.int32, (1, pay_ref.shape[1]), 1)
    row = jnp.zeros((1, pay_ref.shape[1]), F32)
    for b in range(nb):
        row = jnp.where(lane == b, score_ref[b], row)
    pay_ref[0:nb, :] = tok_ref[...].astype(F32)
    pay_ref[nb:nb + 1, :] = row
    pay_ref[nb + 1:8, :] = jnp.zeros((8 - nb - 1, pay_ref.shape[1]), F32)


def main_kernel(dims, n_slots, plan_ref, pos_ref, pay_ref, pm_ref, cs_ref, ga_ref, gm_ref, gf_ref,
                k_ref, v_ref, wq_ref, wk_ref, wv_ref, wo_ref, wg_ref, wu_ref, wd_ref, wvoc_ref,
                cand_ref, new_ref, sib_ref, recv_ref,
                pk0, pk1, pk2, pk3, stage, kv_att, b_q, b_k, b_v, b_o, b_g, b_u, b_d, vbuf,
                payall, resid, qbuf, knew, vnew, pbuf, rbuf, abuf, gbuf, attn,
                s_pl, s_pr, s_pkl, s_pks, s_pkr, s_sib, s_ss, s_sr, s_bs, s_br, s_fs, s_fr,
                s_att, s_w, s_voc, s_1s, s_1r, s_2s, s_2r):
    nb, span, sp_n, hd = dims
    n_layers = ga_ref.shape[0]
    dm = ga_ref.shape[1]
    slots = k_ref.shape[3]
    half = k_ref.shape[2] // 2
    seq = lax.axis_index('sp')
    me = lax.axis_index('beam')
    place = lax.rem(me, span)
    base = me - place
    core = lax.rem(me, CORES)
    other = 1 - core
    rows = CORES * nb
    sib = {'beam': base + lax.div(place, CORES) * CORES + other}
    par = {'beam': base + lax.rem(place + CORES, span)}

    def peer(di, dj):
        return {'beam': base + lax.rem(place + di, span), 'sp': lax.rem(seq + dj, sp_n)}

    everyone = [(di, dj) for di in range(span) for dj in range(sp_n) if (di, dj) != (0, 0)]

    barrier = pltpu.get_barrier_semaphore()
    for di, dj in everyone:
        pl.semaphore_signal(barrier, inc=1, device_id=peer(di, dj), device_id_type=MESH)

    def local(src, dst, sem):
        c = pltpu.make_async_copy(src, dst, sem)
        c.start()
        return c

    def remote(src, dst, ss, rs, dev):
        return pltpu.make_async_remote_copy(src_ref=src, dst_ref=dst, send_sem=ss, recv_sem=rs,
                                            device_id=dev, device_id_type=MESH)

    pks = (pk0, pk1, pk2, pk3)
    chunks = [(src, pl.ds(h * half, half)) for src in (k_ref, v_ref) for h in range(2)]
    pk_local = [local(src.at[core, :, hs], pks[i].at[pl.ds(core * nb, nb)], s_pkl.at[i])
                for i, (src, hs) in enumerate(chunks)]
    w0 = [local(src.at[0], dst.at[0], s_w.at[0, i])
          for i, (src, dst) in enumerate(((wq_ref, b_q), (wk_ref, b_k), (wv_ref, b_v)))]
    att = {}
    for l in range(n_layers):
        for i, src in enumerate((k_ref, v_ref)):
            att[l, i] = local(src.at[l], kv_att.at[l, i], s_att.at[l, i])
    weights = {}
    pairs = ((wq_ref, b_q), (wk_ref, b_k), (wv_ref, b_v), (wo_ref, b_o), (wg_ref, b_g), (wu_ref, b_u), (wd_ref, b_d))
    for l in range(n_layers):
        for i, (src, dst) in enumerate(pairs):
            weights[l, i] = w0[i] if (l == 0 and i < 3) else local(src.at[l], dst.at[l], s_w.at[l, i])
    vocab = wvoc_ref.shape[1]
    n_full = vocab // CHUNK
    tail = vocab - n_full * CHUNK

    def voc_copy(i, slot):
        return pltpu.make_async_copy(wvoc_ref.at[:, pl.ds(i * CHUNK, CHUNK)], vbuf.at[slot], s_voc.at[slot])

    def voc_tail():
        return pltpu.make_async_copy(wvoc_ref.at[:, pl.ds(n_full * CHUNK, tail)],
                                     vbuf.at[n_full % VBUF, :, pl.ds(0, tail)], s_voc.at[n_full % VBUF])

    for i in range(VBUF):
        voc_copy(i, i).start()

    pl.semaphore_wait(barrier, len(everyone))

    pay_out = []
    for di in range(1, span):
        c = remote(pay_ref, payall.at[di], s_pl.at[di], s_pr.at[di], peer(di, 0))
        c.start()
        pay_out.append(c)
    sib_pk = []
    for i, (src, hs) in enumerate(chunks):
        c = remote(src.at[other, :, hs], pks[i].at[pl.ds(core * nb, nb)], s_pks.at[i], s_pkr.at[i], sib)
        c.start()
        sib_pk.append(c)
    sib_rest = []
    for i, src in enumerate((k_ref, v_ref)):
        c = remote(src.at[core], sib_ref.at[core, i], s_ss.at[i], s_sr.at[i], sib)
        c.start()
        sib_rest.append(c)

    def bulk(ch, s):
        dst = recv_ref.at[core, ch // 2, s, pl.ds((ch % 2) * half, half)]
        return remote(stage.at[ch, s], dst, s_bs.at[ch, s], s_br.at[ch, s], par)

    def forward(ch, s):
        ref = recv_ref.at[core, ch // 2, s, pl.ds((ch % 2) * half, half)]
        return remote(ref, ref, s_fs.at[ch, s], s_fr.at[ch, s], sib)

    sib_home = []

    def pack(ch):
        pk_local[ch].wait()
        sib_pk[ch].wait_recv()
        for s in range(n_slots):
            stage[ch, s] = pks[ch][plan_ref[s]]
        hs = pl.ds((ch % 2) * half, half)
        sib_home.append(local(pks[ch].at[pl.ds(other * nb, nb)], sib_ref.at[core, ch // 2, :, hs], s_sib.at[ch]))

    units = [(ch, s) for ch in range(4) for s in range(n_slots)]
    issued = [0]

    def issue(count):
        for ch, s in units[issued[0]:issued[0] + count]:
            bulk(ch, s).start()
        issued[0] = min(len(units), issued[0] + count)

    pack(0)
    issue(min(3, n_slots))

    payall[0] = pay_ref[...]
    for c in pay_out:
        c.wait_recv()
    for i in range(span):
        resid[pl.ds(pl.multiple_of(i * 8, 8), 8), :] = payall[lax.rem(place - i + span, span)]

    lane = lax.broadcasted_iota(jnp.int32, (1, dm), 1)
    low = lax.rem(lane, hd) < hd // 2
    t = pos_ref[0]
    att_scale = hd ** -0.5
    cosv = cs_ref[0:1, :]
    sinv = cs_ref[1:2, :]

    def rope(x):
        swapped = jnp.where(low, pltpu.roll(x, dm - hd // 2, 1), pltpu.roll(x, hd // 2, 1))
        return x * cosv + swapped * sinv

    qw = 256
    hq = qw // hd
    n_quad = dm // qw
    lane_q = lax.broadcasted_iota(jnp.int32, (1, qw), 1)
    head_mask = [lax.div(lane_q, hd) == h for h in range(hq)]
    slot_id = seq * slots + lax.broadcasted_iota(jnp.int32, (1, slots), 1)
    valid = slot_id < t
    pm = pm_ref[...]
    pm4 = jnp.concatenate([pm] * hq, axis=0)
    nrow = pm.shape[0]

    for l in range(n_layers):
        hidden = rms(resid[...], ga_ref[l:l + 1, :])
        for i in range(3):
            weights[l, i].wait()
        q = jnp.dot(hidden, b_q[l], preferred_element_type=F32).astype(BF16).astype(F32)
        k = jnp.dot(hidden, b_k[l], preferred_element_type=F32).astype(BF16).astype(F32)
        v = jnp.dot(hidden, b_v[l], preferred_element_type=F32).astype(BF16).astype(F32)
        q = rope(q).astype(BF16).astype(F32)
        k = rope(k).astype(BF16).astype(F32)
        qbuf[...] = q
        knew[...] = k
        vnew[...] = v
        mine = pl.ds(pl.multiple_of(place * 8, 8), 8)
        new_ref[l, 0] = knew[mine, :]
        new_ref[l, 1] = vnew[mine, :]
        if l == 0:
            for ch in range(1, 4):
                pack(ch)
        att[l, 0].wait()
        att[l, 1].wait()
        for g in range(n_quad):
            gs = pl.ds(g * qw, qw)
            qg = q[:, g * qw:(g + 1) * qw]
            qq = jnp.concatenate([jnp.where(hm, qg, 0.0) for hm in head_mask], axis=0).astype(BF16)
            s = jnp.zeros((hq * nrow, slots), F32)
            for c in range(nb):
                sc = jnp.dot(qq, kv_att[l, 0, c, gs], preferred_element_type=F32)
                s = jnp.where(pm4 == place * 8 + c, sc, s)
            s = jnp.where(valid, s * att_scale, NEG)
            m = jnp.max(s, axis=-1, keepdims=True)
            e = jnp.where(valid, jnp.exp(s - m), 0.0)
            den = jnp.sum(e, axis=-1, keepdims=True)
            acc = jnp.zeros((hq * nrow, qw), F32)
            for c in range(nb):
                ec = jnp.where(pm4 == place * 8 + c, e, 0.0).astype(BF16)
                acc = acc + lax.dot_general(ec, kv_att[l, 1, c, gs], (((1,), (1,)), ((), ())),
                                            preferred_element_type=F32)

            def fold(x):
                y = jnp.zeros((nrow, qw), F32)
                for h in range(hq):
                    y = jnp.where(head_mask[h], x[h * nrow:(h + 1) * nrow], y)
                return y

            for j, x in enumerate((fold(acc), fold(m), fold(den))):
                for w in range(qw // 128):
                    pbuf[l, g * (qw // 128) + w, j] = x[:, w * 128:(w + 1) * 128]
        ex1 = []
        for dj in range(1, sp_n):
            c = remote(pbuf.at[l, lax.rem(seq + dj, sp_n)], rbuf.at[l, dj], s_1s.at[l, dj], s_1r.at[l, dj], peer(0, dj))
            c.start()
            ex1.append(c)
        rbuf[l, 0] = pbuf[l, seq]
        js = pl.ds(pl.multiple_of(seq * 128, 128), 128)
        prod = qbuf[:, js] * knew[:, js]
        lane2 = lax.broadcasted_iota(jnp.int32, (1, 128), 1)
        s_new = jnp.zeros((nrow, 128), F32)
        for h in range(128 // hd):
            hm = lax.div(lane2, hd) == h
            s_new = jnp.where(hm, jnp.sum(jnp.where(hm, prod, 0.0), axis=-1, keepdims=True), s_new)
        s_new = s_new * att_scale
        for c in ex1:
            c.wait_recv()
        m_all = s_new
        for dj in range(sp_n):
            m_all = jnp.maximum(m_all, rbuf[l, dj, 1])
        w_new = jnp.exp(s_new - m_all)
        num = w_new * vnew[:, js]
        den = w_new
        for dj in range(sp_n):
            wj = jnp.exp(rbuf[l, dj, 1] - m_all)
            num = num + wj * rbuf[l, dj, 0]
            den = den + wj * rbuf[l, dj, 2]
        o = jnp.where(lax.div(pm[:, 0:128], 8) == place, num / den, 0.0).astype(BF16)
        abuf[l] = o
        ex2 = []
        for n, (di, dj) in enumerate(everyone):
            c = remote(abuf.at[l], gbuf.at[l, n + 1], s_2s.at[l, n], s_2r.at[l, n], peer(di, dj))
            c.start()
            ex2.append(c)
        issue(4 if l == 0 else len(units))
        gbuf[l, 0] = o
        for i in range(3, 7):
            weights[l, i].wait()
        for c in ex2:
            c.wait_recv()
        for dj in range(sp_n):
            total = gbuf[l, dj].astype(F32)
            for di in range(1, span):
                total = total + gbuf[l, di * sp_n + dj].astype(F32)
            off = pl.multiple_of(lax.rem(seq - dj + sp_n, sp_n) * 128, 128)
            attn[:, pl.ds(off, 128)] = total
        r = resid[...]
        r = r + jnp.dot(attn[...].astype(BF16), b_o[l], preferred_element_type=F32).astype(BF16).astype(F32)
        hidden = rms(r, gm_ref[l:l + 1, :])
        gate = jnp.dot(hidden, b_g[l], preferred_element_type=F32).astype(BF16).astype(F32)
        up = jnp.dot(hidden, b_u[l], preferred_element_type=F32).astype(BF16).astype(F32)
        act = (gate * jax.nn.sigmoid(gate) * up).astype(BF16)
        r = r + jnp.dot(act, b_d[l], preferred_element_type=F32).astype(BF16).astype(F32)
        resid[...] = r
        for c in ex1 + ex2:
            c.wait_send()

    own = resid[pl.ds(pl.multiple_of(place * 8, 8), 8), :]
    hv = rms(own, gf_ref[...])

    @pl.loop(0, n_full)
    def _(i):
        slot = lax.rem(i, VBUF)
        voc_copy(i, slot).wait()
        cand_ref[:, pl.ds(pl.multiple_of(i * CHUNK, CHUNK), CHUNK)] = jnp.dot(
            hv, vbuf[slot], preferred_element_type=F32)

        @pl.when(i + VBUF < n_full)
        def _():
            voc_copy(i + VBUF, slot).start()

        if tail:
            @pl.when(i + VBUF == n_full)
            def _():
                voc_tail().start()

    if tail:
        voc_tail().wait()
        cand_ref[:, pl.ds(n_full * CHUNK, tail)] = jnp.dot(
            hv, vbuf[n_full % VBUF, :, pl.ds(0, tail)], preferred_element_type=F32)

    lg = cand_ref[...]
    mx = jnp.max(lg, axis=-1, keepdims=True)
    lse = jnp.log(jnp.sum(jnp.exp(lg - mx), axis=-1, keepdims=True))
    code = pm_ref[pl.ds(pl.multiple_of(place * 8, 8), 8), 0:128]
    lane1 = lax.broadcasted_iota(jnp.int32, (1, 128), 1)
    score = jnp.zeros((8, 1), F32)
    for i in range(span):
        dev = lax.rem(place - i + span, span)
        srow = payall[i, nb:nb + 1, 0:128]
        score = score + jnp.sum(jnp.where(code == dev * 8 + lane1, srow, 0.0), axis=-1, keepdims=True)
    cand_ref[...] = score + ((cand_ref[...] - mx) - lse)

    for ch in range(4):
        @pl.loop(0, n_slots)
        def _(s, ch=ch):
            bulk(ch, s).wait_recv()
            forward(ch, s).start()
    for c in pay_out + sib_pk + sib_rest:
        c.wait_send()
    for c in sib_rest:
        c.wait_recv()
    for c in sib_home:
        c.wait()
    for ch in range(4):
        @pl.loop(0, n_slots)
        def _(s, ch=ch):
            bulk(ch, s).wait_send()
            forward(ch, s).wait_send()
            ref = recv_ref.at[other, ch // 2, s, pl.ds((ch % 2) * half, half)]
            remote(ref, ref, s_fs.at[ch, s], s_fr.at[ch, s], sib).wait_recv()


def assemble_kernel(dims, plan_ref, pos_ref, new_ref, cand8_ref, k_ref, v_ref, sib_ref, recv_ref,
                    ko_ref, vo_ref, cand_ref, buf, s_in, s_out):
    nb = dims[0]
    rows = CORES * nb
    n_layers = k_ref.shape[0]
    slots = k_ref.shape[3]
    seq = lax.axis_index('sp')
    at = pos_ref[0] - seq * slots
    owns = (at >= 0) & (at < slots)
    order = [(l, i, b) for l in range(n_layers) for i in range(2) for b in range(nb)]
    for u, (l, i, b) in enumerate(order):
        kind = plan_ref[rows + b]
        idx = plan_ref[rows + nb + b]
        src = (k_ref, v_ref)[i]

        @pl.when(kind == 0)
        def _():
            pltpu.make_async_copy(src.at[l, idx], buf.at[u], s_in.at[u]).start()

        @pl.when(kind == 1)
        def _():
            pltpu.make_async_copy(sib_ref.at[l, i, idx], buf.at[u], s_in.at[u]).start()

        @pl.when(kind == 2)
        def _():
            pltpu.make_async_copy(recv_ref.at[l, i, idx], buf.at[u], s_in.at[u]).start()

    cand_ref[...] = cand8_ref[0:nb, :]
    tile = jnp.clip(lax.div(at, 128), 0, slots // 128 - 1)
    lane = lax.broadcasted_iota(jnp.int32, (1, 128), 1)
    outs = []
    for l in range(n_layers):
        for i in range(2):
            cols = jnp.transpose(new_ref[l, i])
            for b in range(nb):
                u = (l * 2 + i) * nb + b
                pltpu.make_async_copy((k_ref, v_ref)[i].at[l, b], buf.at[u], s_in.at[u]).wait()

                @pl.when(owns)
                def _():
                    ts = pl.ds(pl.multiple_of(tile * 128, 128), 128)
                    old = buf[u, :, ts]
                    buf[u, :, ts] = jnp.where(lane == at - tile * 128, cols[:, b:b + 1].astype(BF16), old)

                c = pltpu.make_async_copy(buf.at[u], (ko_ref, vo_ref)[i].at[l, b], s_out.at[u])
                c.start()
                outs.append(c)
    for c in outs:
        c.wait()


def solution(mesh):
    beam_spec = P(('dp', 'beam'))
    row_spec = P(('dp', 'beam'), None)
    cache_spec = P(None, ('dp', 'beam'), 'sp', None, None)
    rep = P()
    sp_n = mesh.shape['sp']

    def local_step(tok_emb, parent, position, beam_score, k_cache, v_cache, w_query, w_key, w_value, w_out,
                   w_gate, w_up, w_down, g_attn, g_mlp, g_final, w_vocab):
        n_layers, nb, slots, heads, hd = k_cache.shape
        width = parent.shape[1]
        span = width // nb
        dm = tok_emb.shape[1]
        ff = w_gate.shape[2]
        vocab = w_vocab.shape[1]
        rows = CORES * nb
        hrow = heads * hd
        kt = k_cache.transpose(0, 1, 3, 4, 2).reshape(n_layers, nb, hrow, slots)
        vt = v_cache.transpose(0, 1, 3, 4, 2).reshape(n_layers, nb, hrow, slots)
        smem = pl.BlockSpec(memory_space=pltpu.SMEM)
        vmem = pl.BlockSpec(memory_space=pltpu.VMEM)
        hbm = pl.BlockSpec(memory_space=pl.ANY)
        sds = jax.ShapeDtypeStruct

        plan, pay, pm = pl.pallas_call(
            functools.partial(plan_kernel, (nb, span)),
            out_shape=(sds((64,), jnp.int32), sds((8, dm), F32), sds((8 * span, slots), jnp.int32)),
            in_specs=[smem, smem, vmem], out_specs=(smem, vmem, vmem),
            scratch_shapes=[pltpu.SMEM((rows,), jnp.int32)],
            name='plan',
        )(parent, beam_score, tok_emb)

        half_dim = hd // 2
        inv_freq = ROPE_BASE ** (-2.0 * jnp.arange(half_dim, dtype=F32) / hd)
        angles = position[0].astype(F32) * inv_freq
        cos_t, sin_t = jnp.cos(angles), jnp.sin(angles)
        cs = jnp.stack([jnp.tile(jnp.concatenate([cos_t, cos_t]), heads),
                        jnp.tile(jnp.concatenate([-sin_t, sin_t]), heads)])

        def main(n_slots, cid, *ops):
            half = hrow // 2
            np_ = dm // 128
            nrow = 8 * span
            dma = pltpu.SemaphoreType.DMA
            scratch = [pltpu.VMEM((rows, half, slots), BF16)] * 4 + [
                pltpu.VMEM((4, n_slots, half, slots), BF16),
                pltpu.VMEM((n_layers, 2, nb, hrow, slots), BF16),
                pltpu.VMEM((n_layers, dm, hrow), BF16),
                pltpu.VMEM((n_layers, dm, hrow), BF16),
                pltpu.VMEM((n_layers, dm, hrow), BF16),
                pltpu.VMEM((n_layers, hrow, dm), BF16),
                pltpu.VMEM((n_layers, dm, ff), BF16),
                pltpu.VMEM((n_layers, dm, ff), BF16),
                pltpu.VMEM((n_layers, ff, dm), BF16),
                pltpu.VMEM((VBUF, dm, CHUNK), BF16),
                pltpu.VMEM((span, 8, dm), F32),
                pltpu.VMEM((nrow, dm), F32),
                pltpu.VMEM((nrow, dm), F32),
                pltpu.VMEM((nrow, dm), F32),
                pltpu.VMEM((nrow, dm), F32),
                pltpu.VMEM((n_layers, np_, 3, nrow, 128), F32),
                pltpu.VMEM((n_layers, sp_n, 3, nrow, 128), F32),
                pltpu.VMEM((n_layers, nrow, 128), BF16),
                pltpu.VMEM((n_layers, span * sp_n, nrow, 128), BF16),
                pltpu.VMEM((nrow, dm), F32),
                dma((span,)), dma((span,)),
                dma((4,)), dma((4,)), dma((4,)), dma((4,)), dma((2,)), dma((2,)),
                dma((4, n_slots)), dma((4, n_slots)), dma((4, n_slots)), dma((4, n_slots)),
                dma((n_layers, 2)), dma((n_layers, 7)), dma((VBUF,)),
                dma((n_layers, sp_n)), dma((n_layers, sp_n)),
                dma((n_layers, span * sp_n)), dma((n_layers, span * sp_n)),
            ]
            return pl.pallas_call(
                functools.partial(main_kernel, (nb, span, sp_n, hd), n_slots),
                out_shape=(sds((8, vocab), F32), sds((n_layers, 2, 8, hrow), F32),
                           sds((n_layers, 2, nb, hrow, slots), BF16),
                           sds((n_layers, 2, rows, hrow, slots), BF16)),
                in_specs=[smem, smem] + [vmem] * 6 + [hbm] * 10,
                out_specs=(vmem, vmem, hbm, hbm),
                scratch_shapes=scratch,
                compiler_params=pltpu.CompilerParams(collective_id=cid, has_side_effects=True,
                                                     vmem_limit_bytes=VMEM_LIMIT),
                name=f'main{n_slots}',
            )(*ops)

        ops = (plan, position, pay, pm, cs, g_attn, g_mlp, g_final.reshape(1, dm), kt, vt,
               w_query, w_key, w_value, w_out, w_gate, w_up, w_down, w_vocab)
        levels = [n for n in LEVELS if n < rows] + [rows]
        most = plan[rows + 2 * nb]
        branch = sum((most > n).astype(jnp.int32) for n in levels[:-1])
        cand8, new, sib, recv = lax.switch(
            branch, [functools.partial(main, n, i) for i, n in enumerate(levels)], *ops)

        ko, vo, cand = pl.pallas_call(
            functools.partial(assemble_kernel, (nb,)),
            out_shape=(sds(kt.shape, BF16), sds(vt.shape, BF16), sds((nb, vocab), F32)),
            in_specs=[smem, smem, vmem, vmem, hbm, hbm, hbm, hbm],
            out_specs=(hbm, hbm, vmem),
            scratch_shapes=[pltpu.VMEM((n_layers * 2 * nb, hrow, slots), BF16),
                            pltpu.SemaphoreType.DMA((n_layers * 2 * nb,)),
                            pltpu.SemaphoreType.DMA((n_layers * 2 * nb,))],
            compiler_params=pltpu.CompilerParams(vmem_limit_bytes=VMEM_LIMIT),
            name='assemble',
        )(plan, position, new, cand8, kt, vt, sib, recv)

        def back(x):
            return x.reshape(n_layers, nb, heads, hd, slots).transpose(0, 1, 4, 2, 3)

        return back(ko), back(vo), cand

    in_specs = (row_spec, P('dp', None), rep, beam_spec, cache_spec, cache_spec) + (rep,) * 11
    return jax.shard_map(local_step, mesh=mesh, in_specs=in_specs, out_specs=(cache_spec, cache_spec, row_spec),
                         check_vma=False)
```

```python
import functools

import jax
import jax.numpy as jnp
from jax import lax
from jax.experimental import pallas as pl
from jax.experimental.pallas import tpu as pltpu
from jax.sharding import PartitionSpec as P

ROPE_BASE = 10000.0
NORM_EPS = 1e-6
NEG = -1e30
CORES = 2
LEVELS = (3, 4, 5, 6)
CHUNK = 2048
VBUF = 10
SPLIT = ((0, 0, 1, 8), (0, 1, 3, 8), (0, 4, 4, 8), (1, 0, 4, 8), (1, 4, 4, 8))
EARLY = 1
VMEM_LIMIT = 64 * 1024 * 1024 - 64 * 1024
MESH = pl.DeviceIdType.MESH
F32 = jnp.float32
BF16 = jnp.bfloat16


def rms(x, g):
    ms = jnp.mean(x * x, axis=-1, keepdims=True)
    return (x * lax.rsqrt(ms + NORM_EPS) * g.astype(F32)).astype(BF16)


def plan_kernel(dims, levels, detour, parent_ref, score_ref, tok_ref, plan_ref, branch_ref, pay_ref, pm_ref, rank_ref):
    nb, span = dims
    rows = CORES * nb
    n_sent, width = parent_ref.shape
    me = lax.axis_index('beam')
    sent = me // span
    place = lax.rem(me, span)
    chip = lax.div(place, CORES)

    def needed(s, to_chip):
        base = (1 - to_chip) * rows
        mask = jnp.int32(0)
        for k in range(rows):
            p = parent_ref[s, to_chip * rows + k] - s * width - base
            mask = mask | jnp.where((p >= 0) & (p < rows), jnp.left_shift(jnp.int32(1), jnp.clip(p, 0, rows - 1)), 0)
        return mask

    def bit(mask, p):
        return jnp.right_shift(mask, p) & 1

    count = {(s, tc): sum(bit(needed(s, tc), p) for p in range(rows)) for s in range(n_sent) for tc in range(2)}
    most = functools.reduce(jnp.maximum, count.values())
    share = most
    if detour:
        share = functools.reduce(jnp.maximum, [most - 1] + [
            lax.div(count[0, tc] + count[1, 1 - tc] + 1, 2) for tc in range(2)])
    out_mask = needed(sent, 1 - chip)
    in_mask = needed(sent, chip)
    for p in range(rows + 1):
        plan_ref[p] = 0
    cnt = jnp.int32(0)
    for p in range(rows):
        @pl.when(bit(out_mask, p) == 1)
        def _(p=p, cnt=cnt):
            plan_ref[cnt] = p
        cnt = cnt + bit(out_mask, p)
    cnt = jnp.int32(0)
    for p in range(rows):
        rank_ref[p] = cnt
        cnt = cnt + bit(in_mask, p)
    for b in range(nb):
        par = parent_ref[sent, place * nb + b] - sent * width
        dev = lax.div(par, nb)
        row = lax.rem(par, nb)
        far = lax.div(dev, CORES) != chip
        slot = rank_ref[jnp.clip(par - (1 - chip) * rows, 0, rows - 1)]
        plan_ref[rows + b] = jnp.where(far, 2, jnp.where(dev == place, 0, 1))
        plan_ref[rows + nb + b] = jnp.where(far, slot, row)
    branch_ref[0] = sum((share > n).astype(jnp.int32) for n in levels[:-1])
    plan_ref[rows + 2 * nb] = sum(bit(out_mask, p) for p in range(rows))
    for i in range(span):
        for b in range(8):
            if b < nb:
                par = parent_ref[sent, i * nb + b] - sent * width
                code = lax.div(par, nb) * 8 + lax.rem(par, nb)
            else:
                code = jnp.int32(-1)
            pm_ref[i * 8 + b:i * 8 + b + 1, :] = jnp.full((1, pm_ref.shape[1]), code, jnp.int32)
    lane = lax.broadcasted_iota(jnp.int32, (1, pay_ref.shape[1]), 1)
    row = jnp.zeros((1, pay_ref.shape[1]), F32)
    for b in range(nb):
        row = jnp.where(lane == b, score_ref[b], row)
    pay_ref[0:nb, :] = tok_ref[...].astype(F32)
    pay_ref[nb:nb + 1, :] = row
    pay_ref[nb + 1:8, :] = jnp.zeros((8 - nb - 1, pay_ref.shape[1]), F32)


def main_kernel(dims, n_slots, detour, plan_ref, pos_ref, pay_ref, pm_ref, cos_ref, sin_ref, ga_ref, gm_ref, gf_ref,
                k_ref, v_ref, wq_ref, wk_ref, wv_ref, wo_ref, wg_ref, wu_ref, wd_ref, wvoc_ref,
                cand_out, new_out, sib_ref, recv_ref, pks, stage, land, spill, spill_in, extra, cand_ref, new_ref, kv_att, b_q, b_k, b_v, b_o, b_g, b_u, b_d, vbuf,
                payall, resid, qbuf, knew, vnew, pbuf, rbuf, abuf, gbuf, attn,
                s_pl, s_pr, s_pkl, s_pks, s_pkr, s_sib, s_ss, s_sr, s_bs, s_br, s_fs, s_fr, s_home, s_os, s_or, s_xs, s_xr, s_out,
                s_att, s_w, s_voc, s_1s, s_1r, s_2s, s_2r):
    nb, span, sp_n, hd = dims
    n_layers = ga_ref.shape[0]
    dm = ga_ref.shape[1]
    slots = k_ref.shape[3]
    hrow = k_ref.shape[2]
    n_vbuf = vbuf.shape[0]
    split = [(kv, hrow // of * a, hrow // of * n) for kv, a, n, of in SPLIT]
    n_ch = len(split)
    seq = lax.axis_index('sp')
    me = lax.axis_index('beam')
    place = lax.rem(me, span)
    base = me - place
    core = lax.rem(me, CORES)
    other = 1 - core
    rows = CORES * nb
    sib = {'beam': base + lax.div(place, CORES) * CORES + other}
    par = {'beam': base + lax.rem(place + CORES, span)}
    chip = lax.div(me, CORES)
    side = {'beam': (span - 1 - chip) * CORES + core}

    def peer(di, dj):
        return {'beam': base + lax.rem(place + di, span), 'sp': lax.rem(seq + dj, sp_n)}

    everyone = [(di, dj) for di in range(span) for dj in range(sp_n) if (di, dj) != (0, 0)]

    barrier = pltpu.get_barrier_semaphore()
    for di, dj in everyone:
        pl.semaphore_signal(barrier, inc=1, device_id=peer(di, dj), device_id_type=MESH)
    if detour:
        pl.semaphore_signal(barrier, inc=1, device_id=side, device_id_type=MESH)

    def local(src, dst, sem):
        c = pltpu.make_async_copy(src, dst, sem)
        c.start()
        return c

    def remote(src, dst, ss, rs, dev):
        return pltpu.make_async_remote_copy(src_ref=src, dst_ref=dst, send_sem=ss, recv_sem=rs,
                                            device_id=dev, device_id_type=MESH)

    src_of = (k_ref, v_ref)
    att = {(role, i): local(src_of[kv].at[lay, :, pl.ds(a, n)], kv_att.at[lay, kv, :, pl.ds(a, n)], s_att.at[role, i])
           for role, lay in enumerate((other, core)) for i, (kv, a, n) in enumerate(split)}
    pk_local = [local(src_of[kv].at[core, :, pl.ds(a, n)], pks[i].at[pl.ds(core * nb, nb)], s_pkl.at[i])
                for i, (kv, a, n) in enumerate(split)]
    w0 = [local(src.at[0], dst.at[0], s_w.at[0, i])
          for i, (src, dst) in enumerate(((wq_ref, b_q), (wk_ref, b_k), (wv_ref, b_v)))]
    weights = {(0, i): c for i, c in enumerate(w0)}
    pairs = ((wq_ref, b_q), (wk_ref, b_k), (wv_ref, b_v), (wo_ref, b_o), (wg_ref, b_g), (wu_ref, b_u), (wd_ref, b_d))

    def load_weights(l, which):
        for i in which:
            weights[l, i] = local(pairs[i][0].at[l], pairs[i][1].at[l], s_w.at[l, i])

    vocab = wvoc_ref.shape[1]
    n_full = vocab // CHUNK
    tail = vocab - n_full * CHUNK

    def voc_copy(i, slot):
        return pltpu.make_async_copy(wvoc_ref.at[:, pl.ds(i * CHUNK, CHUNK)], vbuf.at[slot], s_voc.at[slot])

    def voc_tail():
        return pltpu.make_async_copy(wvoc_ref.at[:, pl.ds(n_full * CHUNK, tail)],
                                     vbuf.at[n_full % n_vbuf, :, pl.ds(0, tail)], s_voc.at[n_full % n_vbuf])

    pl.semaphore_wait(barrier, len(everyone) + int(detour))

    pay_out = []
    for di in range(1, span):
        c = remote(pay_ref, payall.at[di], s_pl.at[di], s_pr.at[di], peer(di, 0))
        c.start()
        pay_out.append(c)
    sib_pk = []
    for i, (kv, a, n) in enumerate(split):
        att[0, i].wait()
        c = remote(kv_att.at[other, kv, :, pl.ds(a, n)], pks[i].at[pl.ds(core * nb, nb)], s_pks.at[i], s_pkr.at[i], sib)
        c.start()
        sib_pk.append(c)
    sib_rest = []
    for i, src in enumerate((k_ref, v_ref)):
        c = remote(src.at[core], sib_ref.at[core, i], s_ss.at[i], s_sr.at[i], sib)
        c.start()
        sib_rest.append(c)

    def bulk(ch, s):
        return remote(stage[ch].at[s], land[ch].at[s], s_bs.at[ch, s], s_br.at[ch, s], par)

    def home(lay, ch, s):
        kv, a, n = split[ch]
        return recv_ref.at[lay, kv, s, pl.ds(a, n)]

    def forward(ch, s):
        return remote(land[ch].at[s], home(core, ch, s), s_fs.at[ch, s], s_fr.at[ch, s], sib)

    def settle(ch, s):
        return pltpu.make_async_copy(land[ch].at[s], home(core, ch, s), s_home.at[ch, s])

    def spill_to(ch):
        return remote(spill[ch], spill_in[ch], s_os.at[ch], s_or.at[ch], side)

    def hand_over(ch):
        return remote(land[ch].at[n_slots - 1], extra[ch], s_xs.at[ch], s_xr.at[ch], side)

    def forward_extra(ch):
        return remote(extra[ch], home(core, ch, n_slots), s_fs.at[ch, n_slots], s_fr.at[ch, n_slots], sib)

    def settle_extra(ch):
        return pltpu.make_async_copy(extra[ch], home(core, ch, n_slots), s_home.at[ch, n_slots])

    last = n_slots - 1 if detour else n_slots
    sib_home = []

    def pack(ch):
        kv, a, n = split[ch]
        pk_local[ch].wait()
        sib_pk[ch].wait_recv()
        if detour:
            spill[ch][...] = pks[ch][plan_ref[n_slots]]
        for s in range(last):
            stage[ch][s] = pks[ch][plan_ref[s]]
        if detour:
            spill_to(ch).start()
        sib_home.append(local(pks[ch].at[pl.ds(other * nb, nb)], sib_ref.at[core, kv, :, pl.ds(a, n)], s_sib.at[ch]))

    def pack_last(ch):
        spill_to(ch).wait_recv()
        mine = plan_ref[rows + 2 * nb] >= n_slots
        own = pks[ch][plan_ref[n_slots - 1]]
        stage[ch][n_slots - 1] = jnp.where(mine, own, spill_in[ch][...])

    queue = []

    def send(ch, lo=0, hi=None):
        hi = last if hi is None else min(hi, last)
        for s in range(lo, hi):
            bulk(ch, s).start()
        if lo < hi:
            queue.append((ch, lo, hi))

    def send_last(*chs):
        if detour:
            for ch in chs:
                pack_last(ch)
            for ch in chs:
                bulk(ch, n_slots - 1).start()
                queue.append((ch, n_slots - 1, n_slots))

    def drain(count=None):
        todo = queue[:count]
        del queue[:count]
        for ch, lo, hi in todo:
            @pl.loop(lo, hi)
            def _(s, ch=ch):
                bulk(ch, s).wait_recv()
                forward(ch, s).start()
                settle(ch, s).start()

            if detour and hi == n_slots:
                hand_over(ch).start()

    for ch in range(2):
        pack(ch)
        send(ch)

    payall[0] = pay_ref[...]
    for c in pay_out:
        c.wait_recv()
    for i in range(span):
        resid[pl.ds(pl.multiple_of(i * 8, 8), 8), :] = payall[lax.rem(place - i + span, span)]

    lane = lax.broadcasted_iota(jnp.int32, (1, dm), 1)
    low = lax.rem(lane, hd) < hd // 2
    t = pos_ref[0]
    att_scale = hd ** -0.5
    cosv = cos_ref[...]
    sinv = sin_ref[...]

    def rope(x):
        swapped = jnp.where(low, pltpu.roll(x, dm - hd // 2, 1), pltpu.roll(x, hd // 2, 1))
        return x * cosv + swapped * sinv

    qw = 256
    hq = qw // hd
    n_quad = dm // qw
    lane_q = lax.broadcasted_iota(jnp.int32, (1, qw), 1)
    head_mask = [lax.div(lane_q, hd) == h for h in range(hq)]
    low_q = lax.rem(lane_q, hd) < hd // 2
    slot_id = seq * slots + lax.broadcasted_iota(jnp.int32, (1, slots), 1)
    valid = slot_id < t
    pm = pm_ref[...]
    pm4 = jnp.concatenate([pm] * hq, axis=0)
    nrow = pm.shape[0]

    for l in range(n_layers):
        hidden = rms(resid[...], ga_ref[l:l + 1, :])
        for i in range(3):
            weights[l, i].wait()
        q = jnp.dot(hidden, b_q[l], preferred_element_type=F32).astype(BF16).astype(F32)
        k = jnp.dot(hidden, b_k[l], preferred_element_type=F32).astype(BF16).astype(F32)
        v = jnp.dot(hidden, b_v[l], preferred_element_type=F32).astype(BF16).astype(F32)
        q = rope(q).astype(BF16).astype(F32)
        k = rope(k).astype(BF16).astype(F32)
        qbuf[...] = q
        knew[...] = k
        vnew[...] = v
        mine = pl.ds(pl.multiple_of(place * 8, 8), 8)
        new_ref[l, 0] = knew[mine, :]
        new_ref[l, 1] = vnew[mine, :]
        if l == 0:
            for ch in range(2, n_ch):
                pack(ch)
            send(2, 0, EARLY)
            for i in range(n_ch):
                att[1, i].wait()
            load_weights(0, range(3, 7))
            load_weights(1, range(0, 3))
            load_weights(1, range(3, 7))
            for i in range(n_vbuf):
                voc_copy(i, i).start()
        for g in range(n_quad):
            gs = pl.ds(g * qw, qw)
            qg = q[:, g * qw:(g + 1) * qw]
            qq = jnp.concatenate([jnp.where(hm, qg, 0.0) for hm in head_mask], axis=0).astype(BF16)
            s = jnp.zeros((hq * nrow, slots), F32)
            for c in range(nb):
                sc = jnp.dot(qq, kv_att[l, 0, c, gs], preferred_element_type=F32)
                s = jnp.where(pm4 == place * 8 + c, sc, s)
            s = jnp.where(valid, s * att_scale, NEG)
            m = jnp.max(s, axis=-1, keepdims=True)
            e = jnp.where(valid, jnp.exp(s - m), 0.0)
            den = jnp.sum(e, axis=-1, keepdims=True)
            acc = jnp.zeros((hq * nrow, qw), F32)
            for c in range(nb):
                ec = jnp.where(pm4 == place * 8 + c, e, 0.0).astype(BF16)
                acc = acc + lax.dot_general(ec, kv_att[l, 1, c, gs], (((1,), (1,)), ((), ())),
                                            preferred_element_type=F32)

            def fold(x):
                y = jnp.zeros((nrow, qw), F32)
                for h in range(hq):
                    y = jnp.where(head_mask[h], x[h * nrow:(h + 1) * nrow], y)
                return y

            for j, x in enumerate((fold(acc), jnp.where(low_q, fold(m), fold(den)))):
                for w in range(qw // 128):
                    pbuf[l, g * (qw // 128) + w, j] = x[:, w * 128:(w + 1) * 128]
        ex1 = []
        for dj in range(1, sp_n):
            c = remote(pbuf.at[l, lax.rem(seq + dj, sp_n)], rbuf.at[l, dj], s_1s.at[l, dj], s_1r.at[l, dj], peer(0, dj))
            c.start()
            ex1.append(c)
        rbuf[l, 0] = pbuf[l, seq]
        js = pl.ds(pl.multiple_of(seq * 128, 128), 128)
        prod = qbuf[:, js] * knew[:, js]
        lane2 = lax.broadcasted_iota(jnp.int32, (1, 128), 1)
        s_new = jnp.zeros((nrow, 128), F32)
        for h in range(128 // hd):
            hm = lax.div(lane2, hd) == h
            s_new = jnp.where(hm, jnp.sum(jnp.where(hm, prod, 0.0), axis=-1, keepdims=True), s_new)
        s_new = s_new * att_scale
        for c in ex1:
            c.wait_recv()
        low2 = lax.rem(lane2, hd) < hd // 2
        ml = [rbuf[l, dj, 1] for dj in range(sp_n)]
        maxes = [jnp.where(low2, x, pltpu.roll(x, hd // 2, 1)) for x in ml]
        sums = [jnp.where(low2, pltpu.roll(x, 128 - hd // 2, 1), x) for x in ml]
        m_all = s_new
        for x in maxes:
            m_all = jnp.maximum(m_all, x)
        w_new = jnp.exp(s_new - m_all)
        num = w_new * vnew[:, js]
        den = w_new
        for dj in range(sp_n):
            wj = jnp.exp(maxes[dj] - m_all)
            num = num + wj * rbuf[l, dj, 0]
            den = den + wj * sums[dj]
        o = jnp.where(lax.div(pm[:, 0:128], 8) == place, num / den, 0.0).astype(BF16)
        abuf[l] = o
        ex2 = []
        for n, (di, dj) in enumerate(everyone):
            c = remote(abuf.at[l], gbuf.at[l, n + 1], s_2s.at[l, n], s_2r.at[l, n], peer(di, dj))
            c.start()
            ex2.append(c)
        if l == 0:
            send_last(0, 1, 2)
            send(2, EARLY)
        else:
            send_last(3, 4)
            send(3)
            send(4)
        if l == 1:
            drain(2)
        gbuf[l, 0] = o
        for i in range(3, 7):
            weights[l, i].wait()
        for c in ex2:
            c.wait_recv()
        for dj in range(sp_n):
            total = gbuf[l, dj].astype(F32)
            for di in range(1, span):
                total = total + gbuf[l, di * sp_n + dj].astype(F32)
            off = pl.multiple_of(lax.rem(seq - dj + sp_n, sp_n) * 128, 128)
            attn[:, pl.ds(off, 128)] = total
        r = resid[...]
        r = r + jnp.dot(attn[...].astype(BF16), b_o[l], preferred_element_type=F32).astype(BF16).astype(F32)
        hidden = rms(r, gm_ref[l:l + 1, :])
        gate = jnp.dot(hidden, b_g[l], preferred_element_type=F32).astype(BF16).astype(F32)
        up = jnp.dot(hidden, b_u[l], preferred_element_type=F32).astype(BF16).astype(F32)
        act = (gate * jax.nn.sigmoid(gate) * up).astype(BF16)
        r = r + jnp.dot(act, b_d[l], preferred_element_type=F32).astype(BF16).astype(F32)
        resid[...] = r
        for c in ex1 + ex2:
            c.wait_send()

    new_home = local(new_ref, new_out, s_out.at[0])
    drain(max(0, len(queue) - (4 if detour else 2)))
    own = resid[pl.ds(pl.multiple_of(place * 8, 8), 8), :]
    hv = rms(own, gf_ref[...].astype(F32).reshape(1, dm))

    @pl.loop(0, n_full)
    def _(i):
        slot = lax.rem(i, n_vbuf)
        voc_copy(i, slot).wait()
        cand_ref[:, pl.ds(pl.multiple_of(i * CHUNK, CHUNK), CHUNK)] = jnp.dot(
            hv, vbuf[slot], preferred_element_type=F32)

        @pl.when(i + n_vbuf < n_full)
        def _():
            voc_copy(i + n_vbuf, slot).start()

        if tail:
            @pl.when(i + n_vbuf == n_full)
            def _():
                voc_tail().start()

    if tail:
        voc_tail().wait()
        cand_ref[:, pl.ds(n_full * CHUNK, tail)] = jnp.dot(
            hv, vbuf[n_full % n_vbuf, :, pl.ds(0, tail)], preferred_element_type=F32)

    lg = cand_ref[...]
    mx = jnp.max(lg, axis=-1, keepdims=True)
    lse = jnp.log(jnp.sum(jnp.exp(lg - mx), axis=-1, keepdims=True))
    code = pm_ref[pl.ds(pl.multiple_of(place * 8, 8), 8), 0:128]
    lane1 = lax.broadcasted_iota(jnp.int32, (1, 128), 1)
    score = jnp.zeros((8, 1), F32)
    for i in range(span):
        dev = lax.rem(place - i + span, span)
        srow = payall[i, nb:nb + 1, 0:128]
        score = score + jnp.sum(jnp.where(code == dev * 8 + lane1, srow, 0.0), axis=-1, keepdims=True)
    cand_ref[...] = score + ((cand_ref[...] - mx) - lse)

    cand_home = local(cand_ref, cand_out, s_out.at[1])
    drain()
    if detour:
        for ch in range(n_ch):
            hand_over(ch).wait_recv()
            forward_extra(ch).start()
            settle_extra(ch).start()
    for c in pay_out + sib_pk + sib_rest:
        c.wait_send()
    for c in sib_rest:
        c.wait_recv()
    for c in sib_home + [new_home, cand_home]:
        c.wait()
    for ch in range(n_ch):
        @pl.loop(0, n_slots)
        def _(s, ch=ch):
            bulk(ch, s).wait_send()
            settle(ch, s).wait()
            forward(ch, s).wait_send()
            remote(land[ch].at[s], home(other, ch, s), s_fs.at[ch, s], s_fr.at[ch, s], sib).wait_recv()
        if detour:
            spill_to(ch).wait_send()
            hand_over(ch).wait_send()
            settle_extra(ch).wait()
            forward_extra(ch).wait_send()
            remote(extra[ch], home(other, ch, n_slots), s_fs.at[ch, n_slots], s_fr.at[ch, n_slots], sib).wait_recv()


def assemble_kernel(dims, plan_ref, pos_ref, new_ref, cand8_ref, k_ref, v_ref, sib_ref, recv_ref,
                    ko_ref, vo_ref, cand_ref, buf, cbuf, c6, nbuf, s_in, s_out, s_c):
    nb = dims[0]
    rows = CORES * nb
    n_layers = k_ref.shape[0]
    slots = k_ref.shape[3]
    seq = lax.axis_index('sp')
    at = pos_ref[0] - seq * slots
    owns = (at >= 0) & (at < slots)
    new_in = pltpu.make_async_copy(new_ref, nbuf, s_c.at[0])
    new_in.start()
    order = [(l, i, b) for l in range(n_layers) for i in range(2) for b in range(nb)]
    for u, (l, i, b) in enumerate(order):
        kind = plan_ref[rows + b]
        idx = plan_ref[rows + nb + b]
        src = (k_ref, v_ref)[i]

        @pl.when(kind == 0)
        def _():
            pltpu.make_async_copy(src.at[l, idx], buf.at[u], s_in.at[u]).start()

        @pl.when(kind == 1)
        def _():
            pltpu.make_async_copy(sib_ref.at[l, i, idx], buf.at[u], s_in.at[u]).start()

        @pl.when(kind == 2)
        def _():
            pltpu.make_async_copy(recv_ref.at[l, i, idx], buf.at[u], s_in.at[u]).start()

    cand_in = pltpu.make_async_copy(cand8_ref, cbuf, s_c.at[1])
    cand_in.start()
    new_in.wait()
    tile = jnp.clip(lax.div(at, 128), 0, slots // 128 - 1)
    lane = lax.broadcasted_iota(jnp.int32, (1, 128), 1)
    outs = []
    for l in range(n_layers):
        for i in range(2):
            cols = jnp.transpose(nbuf[l, i])
            for b in range(nb):
                u = (l * 2 + i) * nb + b
                pltpu.make_async_copy((k_ref, v_ref)[i].at[l, b], buf.at[u], s_in.at[u]).wait()

                @pl.when(owns)
                def _():
                    ts = pl.ds(pl.multiple_of(tile * 128, 128), 128)
                    old = buf[u, :, ts]
                    buf[u, :, ts] = jnp.where(lane == at - tile * 128, cols[:, b:b + 1].astype(BF16), old)

                c = pltpu.make_async_copy(buf.at[u], (ko_ref, vo_ref)[i].at[l, b], s_out.at[u])
                c.start()
                outs.append(c)
    cand_in.wait()
    c6[...] = cbuf[0:nb, :]
    cand_back = pltpu.make_async_copy(c6, cand_ref, s_c.at[2])
    cand_back.start()
    for c in outs + [cand_back]:
        c.wait()


def solution(mesh):
    beam_spec = P(('dp', 'beam'))
    row_spec = P(('dp', 'beam'), None)
    cache_spec = P(None, ('dp', 'beam'), 'sp', None, None)
    rep = P()
    sp_n = mesh.shape['sp']

    def local_step(tok_emb, parent, position, beam_score, k_cache, v_cache, w_query, w_key, w_value, w_out,
                   w_gate, w_up, w_down, g_attn, g_mlp, g_final, w_vocab):
        n_layers, nb, slots, heads, hd = k_cache.shape
        width = parent.shape[1]
        span = width // nb
        dm = tok_emb.shape[1]
        ff = w_gate.shape[2]
        vocab = w_vocab.shape[1]
        rows = CORES * nb
        hrow = heads * hd
        kt = k_cache.transpose(0, 1, 3, 4, 2).reshape(n_layers, nb, hrow, slots)
        vt = v_cache.transpose(0, 1, 3, 4, 2).reshape(n_layers, nb, hrow, slots)
        smem = pl.BlockSpec(memory_space=pltpu.SMEM)
        vmem = pl.BlockSpec(memory_space=pltpu.VMEM)
        hbm = pl.BlockSpec(memory_space=pl.ANY)
        sds = jax.ShapeDtypeStruct

        levels = [n for n in LEVELS if n < rows] + [rows]
        n_chips = mesh.shape['beam'] // CORES
        detour = parent.shape[0] == 2 and span == 2 * CORES and n_chips == 4
        plan, branch, pay, pm = pl.pallas_call(
            functools.partial(plan_kernel, (nb, span), levels, detour),
            out_shape=(sds((64,), jnp.int32), sds((1,), jnp.int32), sds((8, dm), F32), sds((8 * span, slots), jnp.int32)),
            in_specs=[smem, smem, vmem], out_specs=(smem, smem, vmem, vmem),
            scratch_shapes=[pltpu.SMEM((rows,), jnp.int32)],
            name='plan',
        )(parent, beam_score, tok_emb)

        half_dim = hd // 2
        lane = lax.broadcasted_iota(jnp.int32, (1, hrow), 1)
        inv_freq = ROPE_BASE ** (-2.0 * (lane % half_dim).astype(F32) / hd)
        angles = position[0].astype(F32) * inv_freq
        cos_t = jnp.cos(angles)
        sin_t = jnp.where(lane % hd < half_dim, -1.0, 1.0) * jnp.sin(angles)

        def main(n_slots, cid, *ops):
            np_ = dm // 128
            nrow = 8 * span
            dma = pltpu.SemaphoreType.DMA
            n_vbuf = VBUF if 2 * n_slots <= rows else VBUF // 2
            sizes = [hrow // of * n for _, _, n, of in SPLIT]
            nch = len(sizes)
            scratch = [
                [pltpu.VMEM((rows, n, slots), BF16) for n in sizes],
                [pltpu.VMEM((n_slots, n, slots), BF16) for n in sizes],
                [pltpu.VMEM((n_slots, n, slots), BF16) for n in sizes],
                [pltpu.VMEM((n, slots), BF16) for n in sizes],
                [pltpu.VMEM((n, slots), BF16) for n in sizes],
                [pltpu.VMEM((n, slots), BF16) for n in sizes],
                pltpu.VMEM((8, vocab), F32), pltpu.VMEM((n_layers, 2, 8, hrow), F32),
                pltpu.VMEM((n_layers, 2, nb, hrow, slots), BF16),
                pltpu.VMEM((n_layers, dm, hrow), BF16),
                pltpu.VMEM((n_layers, dm, hrow), BF16),
                pltpu.VMEM((n_layers, dm, hrow), BF16),
                pltpu.VMEM((n_layers, hrow, dm), BF16),
                pltpu.VMEM((n_layers, dm, ff), BF16),
                pltpu.VMEM((n_layers, dm, ff), BF16),
                pltpu.VMEM((n_layers, ff, dm), BF16),
                pltpu.VMEM((n_vbuf, dm, CHUNK), BF16),
                pltpu.VMEM((span, 8, dm), F32),
                pltpu.VMEM((nrow, dm), F32),
                pltpu.VMEM((nrow, dm), F32),
                pltpu.VMEM((nrow, dm), F32),
                pltpu.VMEM((nrow, dm), F32),
                pltpu.VMEM((n_layers, np_, 2, nrow, 128), F32),
                pltpu.VMEM((n_layers, sp_n, 2, nrow, 128), F32),
                pltpu.VMEM((n_layers, nrow, 128), BF16),
                pltpu.VMEM((n_layers, span * sp_n, nrow, 128), BF16),
                pltpu.VMEM((nrow, dm), F32),
                dma((span,)), dma((span,)),
                dma((nch,)), dma((nch,)), dma((nch,)), dma((nch,)), dma((2,)), dma((2,)),
                dma((nch, n_slots)), dma((nch, n_slots)), dma((nch, n_slots + 1)), dma((nch, n_slots + 1)),
                dma((nch, n_slots + 1)), dma((nch,)), dma((nch,)), dma((nch,)), dma((nch,)), dma((2,)),
                dma((2, nch)), dma((n_layers, 7)), dma((n_vbuf,)),
                dma((n_layers, sp_n)), dma((n_layers, sp_n)),
                dma((n_layers, span * sp_n)), dma((n_layers, span * sp_n)),
            ]
            return pl.pallas_call(
                functools.partial(main_kernel, (nb, span, sp_n, hd), n_slots, detour and n_slots < rows),
                out_shape=(sds((8, vocab), F32), sds((n_layers, 2, 8, hrow), F32),
                           sds((n_layers, 2, nb, hrow, slots), BF16),
                           sds((n_layers, 2, rows, hrow, slots), BF16)),
                in_specs=[smem, smem] + [vmem] * 7 + [hbm] * 10,
                out_specs=(hbm, hbm, hbm, hbm),
                scratch_shapes=scratch,
                compiler_params=pltpu.CompilerParams(collective_id=cid, has_side_effects=True,
                                                     vmem_limit_bytes=VMEM_LIMIT),
                name=f'main{n_slots}',
            )(*ops)

        ops = (plan, position, pay, pm, cos_t, sin_t, g_attn, g_mlp, g_final, kt, vt,
               w_query, w_key, w_value, w_out, w_gate, w_up, w_down, w_vocab)
        cand8, new, sib, recv = lax.switch(
            branch[0], [functools.partial(main, n, i) for i, n in enumerate(levels)], *ops)

        ko, vo, cand = pl.pallas_call(
            functools.partial(assemble_kernel, (nb,)),
            out_shape=(sds(kt.shape, BF16), sds(vt.shape, BF16), sds((nb, vocab), F32)),
            in_specs=[smem, smem, hbm, hbm, hbm, hbm, hbm, hbm],
            out_specs=(hbm, hbm, hbm),
            scratch_shapes=[pltpu.VMEM((n_layers * 2 * nb, hrow, slots), BF16),
                            pltpu.VMEM((8, vocab), F32), pltpu.VMEM((nb, vocab), F32), pltpu.VMEM((n_layers, 2, 8, hrow), F32),
                            pltpu.SemaphoreType.DMA((n_layers * 2 * nb,)),
                            pltpu.SemaphoreType.DMA((n_layers * 2 * nb,)), pltpu.SemaphoreType.DMA((3,))],
            compiler_params=pltpu.CompilerParams(vmem_limit_bytes=VMEM_LIMIT),
            name='assemble',
        )(plan, position, new, cand8, kt, vt, sib, recv)

        def back(x):
            return x.reshape(n_layers, nb, heads, hd, slots).transpose(0, 1, 4, 2, 3)

        return back(ko), back(vo), cand

    in_specs = (row_spec, P('dp', None), rep, beam_spec, cache_spec, cache_spec) + (rep,) * 11
    return jax.shard_map(local_step, mesh=mesh, in_specs=in_specs, out_specs=(cache_spec, cache_spec, row_spec),
                         check_vma=False)
```

```python
import functools

import jax
import jax.numpy as jnp
from jax import lax
from jax.experimental import pallas as pl
from jax.experimental.pallas import tpu as pltpu
from jax.sharding import PartitionSpec as P

ROPE_BASE = 10000.0
NORM_EPS = 1e-6
NEG = -1e30
CORES = 2
LEVELS = (3, 4, 5, 6)
CHUNK = 2048
VBUF = 10
FF_PARTS = 2
SPLIT = ((0, 0, 1, 8), (0, 1, 3, 8), (0, 4, 4, 8), (1, 0, 4, 8), (1, 4, 4, 8))
EARLY = 1
VMEM_LIMIT = 64 * 1024 * 1024 - 64 * 1024
MESH = pl.DeviceIdType.MESH
F32 = jnp.float32
BF16 = jnp.bfloat16


def rms(x, g):
    ms = jnp.mean(x * x, axis=-1, keepdims=True)
    return (x * lax.rsqrt(ms + NORM_EPS) * g.astype(F32)).astype(BF16)


def plan_kernel(dims, levels, detour, parent_ref, score_ref, tok_ref, plan_ref, branch_ref, pay_ref, pm_ref, rank_ref):
    nb, span = dims
    rows = CORES * nb
    n_sent, width = parent_ref.shape
    me = lax.axis_index('beam')
    sent = me // span
    place = lax.rem(me, span)
    chip = lax.div(place, CORES)

    def needed(s, to_chip):
        base = (1 - to_chip) * rows
        mask = jnp.int32(0)
        for k in range(rows):
            p = parent_ref[s, to_chip * rows + k] - s * width - base
            mask = mask | jnp.where((p >= 0) & (p < rows), jnp.left_shift(jnp.int32(1), jnp.clip(p, 0, rows - 1)), 0)
        return mask

    def bit(mask, p):
        return jnp.right_shift(mask, p) & 1

    count = {(s, tc): sum(bit(needed(s, tc), p) for p in range(rows)) for s in range(n_sent) for tc in range(2)}
    most = functools.reduce(jnp.maximum, count.values())
    share = most
    if detour:
        share = functools.reduce(jnp.maximum, [most - 1] + [
            lax.div(count[0, tc] + count[1, 1 - tc] + 1, 2) for tc in range(2)])
    out_mask = needed(sent, 1 - chip)
    in_mask = needed(sent, chip)
    for p in range(rows + 1):
        plan_ref[p] = 0
    cnt = jnp.int32(0)
    for p in range(rows):
        @pl.when(bit(out_mask, p) == 1)
        def _(p=p, cnt=cnt):
            plan_ref[cnt] = p
        cnt = cnt + bit(out_mask, p)
    cnt = jnp.int32(0)
    for p in range(rows):
        rank_ref[p] = cnt
        cnt = cnt + bit(in_mask, p)
    for b in range(nb):
        par = parent_ref[sent, place * nb + b] - sent * width
        dev = lax.div(par, nb)
        row = lax.rem(par, nb)
        far = lax.div(dev, CORES) != chip
        slot = rank_ref[jnp.clip(par - (1 - chip) * rows, 0, rows - 1)]
        plan_ref[rows + b] = jnp.where(far, 2, jnp.where(dev == place, 0, 1))
        plan_ref[rows + nb + b] = jnp.where(far, slot, row)
    branch_ref[0] = sum((share > n).astype(jnp.int32) for n in levels[:-1])
    plan_ref[rows + 2 * nb] = sum(bit(out_mask, p) for p in range(rows))
    for i in range(span):
        for b in range(8):
            if b < nb:
                par = parent_ref[sent, i * nb + b] - sent * width
                code = lax.div(par, nb) * 8 + lax.rem(par, nb)
            else:
                code = jnp.int32(-1)
            pm_ref[i * 8 + b:i * 8 + b + 1, :] = jnp.full((1, pm_ref.shape[1]), code, jnp.int32)
    lane = lax.broadcasted_iota(jnp.int32, (1, pay_ref.shape[1]), 1)
    row = jnp.zeros((1, pay_ref.shape[1]), F32)
    for b in range(nb):
        row = jnp.where(lane == b, score_ref[b], row)
    pay_ref[0:nb, :] = tok_ref[...].astype(F32)
    pay_ref[nb:nb + 1, :] = row
    pay_ref[nb + 1:8, :] = jnp.zeros((8 - nb - 1, pay_ref.shape[1]), F32)


def main_kernel(dims, n_slots, detour, plan_ref, pos_ref, pay_ref, pm_ref, cos_ref, sin_ref, ga_ref, gm_ref, gf_ref,
                k_ref, v_ref, wq_ref, wk_ref, wv_ref, wo_ref, wg_ref, wu_ref, wd_ref, wvoc_ref,
                cand_out, new_out, sib_ref, recv_ref, pks, stage, land, spill, spill_in, extra, cand_ref, new_ref, kv_att, b_q, b_k, b_v, b_o, b_g, b_u, b_d, vbuf,
                payall, resid, qbuf, knew, vnew, pbuf, rbuf, abuf, gbuf, attn,
                s_pl, s_pr, s_pkl, s_pks, s_pkr, s_sib, s_ss, s_sr, s_bs, s_br, s_fs, s_fr, s_home, s_os, s_or, s_xs, s_xr, s_out,
                s_att, s_w, s_voc, s_1s, s_1r, s_2s, s_2r):
    nb, span, sp_n, hd = dims
    n_layers = ga_ref.shape[0]
    dm = ga_ref.shape[1]
    slots = k_ref.shape[3]
    hrow = k_ref.shape[2]
    n_vbuf = vbuf.shape[0]
    split = [(kv, hrow // of * a, hrow // of * n) for kv, a, n, of in SPLIT]
    n_ch = len(split)
    seq = lax.axis_index('sp')
    me = lax.axis_index('beam')
    place = lax.rem(me, span)
    base = me - place
    core = lax.rem(me, CORES)
    other = 1 - core
    rows = CORES * nb
    sib = {'beam': base + lax.div(place, CORES) * CORES + other}
    par = {'beam': base + lax.rem(place + CORES, span)}
    chip = lax.div(me, CORES)
    side = {'beam': (span - 1 - chip) * CORES + core}

    def peer(di, dj):
        return {'beam': base + lax.rem(place + di, span), 'sp': lax.rem(seq + dj, sp_n)}

    everyone = [(di, dj) for di in range(span) for dj in range(sp_n) if (di, dj) != (0, 0)]

    barrier = pltpu.get_barrier_semaphore()
    for di, dj in everyone:
        pl.semaphore_signal(barrier, inc=1, device_id=peer(di, dj), device_id_type=MESH)
    if detour:
        pl.semaphore_signal(barrier, inc=1, device_id=side, device_id_type=MESH)

    def local(src, dst, sem):
        c = pltpu.make_async_copy(src, dst, sem)
        c.start()
        return c

    def remote(src, dst, ss, rs, dev):
        return pltpu.make_async_remote_copy(src_ref=src, dst_ref=dst, send_sem=ss, recv_sem=rs,
                                            device_id=dev, device_id_type=MESH)

    src_of = (k_ref, v_ref)
    att, pk_local = {}, []

    def load_cache(role, lay, i):
        kv, a, n = split[i]
        att[role, i] = local(src_of[kv].at[lay, :, pl.ds(a, n)], kv_att.at[lay, kv, :, pl.ds(a, n)], s_att.at[role, i])

    for i, (kv, a, n) in enumerate(split):
        load_cache(0, other, i)
        pk_local.append(local(src_of[kv].at[core, :, pl.ds(a, n)], pks[i].at[pl.ds(core * nb, nb)], s_pkl.at[i]))
    w0 = [local(src.at[0], dst.at[0], s_w.at[0, i])
          for i, (src, dst) in enumerate(((wq_ref, b_q), (wk_ref, b_k), (wv_ref, b_v)))]
    for i in range(n_ch):
        load_cache(1, core, i)
    weights = {(0, i): c for i, c in enumerate(w0)}
    pairs = ((wq_ref, b_q), (wk_ref, b_k), (wv_ref, b_v), (wo_ref, b_o), (wg_ref, b_g), (wu_ref, b_u), (wd_ref, b_d))

    def load_weights(l, which):
        for i in which:
            weights[l, i] = local(pairs[i][0].at[l], pairs[i][1].at[l], s_w.at[l, i])

    vocab = wvoc_ref.shape[1]
    n_full = vocab // CHUNK
    tail = vocab - n_full * CHUNK

    def voc_copy(i, slot):
        return pltpu.make_async_copy(wvoc_ref.at[:, pl.ds(i * CHUNK, CHUNK)], vbuf.at[slot], s_voc.at[slot])

    def voc_tail():
        return pltpu.make_async_copy(wvoc_ref.at[:, pl.ds(n_full * CHUNK, tail)],
                                     vbuf.at[n_full % n_vbuf, :, pl.ds(0, tail)], s_voc.at[n_full % n_vbuf])

    pl.semaphore_wait(barrier, len(everyone) + int(detour))

    pay_out = []
    for di in range(1, span):
        c = remote(pay_ref, payall.at[di], s_pl.at[di], s_pr.at[di], peer(di, 0))
        c.start()
        pay_out.append(c)
    sib_pk = []
    for i, (kv, a, n) in enumerate(split):
        att[0, i].wait()
        c = remote(kv_att.at[other, kv, :, pl.ds(a, n)], pks[i].at[pl.ds(core * nb, nb)], s_pks.at[i], s_pkr.at[i], sib)
        c.start()
        sib_pk.append(c)
    sib_rest = []
    for i, src in enumerate((k_ref, v_ref)):
        c = remote(src.at[core], sib_ref.at[core, i], s_ss.at[i], s_sr.at[i], sib)
        c.start()
        sib_rest.append(c)

    def bulk(ch, s):
        return remote(stage[ch].at[s], land[ch].at[s], s_bs.at[ch, s], s_br.at[ch, s], par)

    def home(lay, ch, s):
        kv, a, n = split[ch]
        return recv_ref.at[lay, kv, s, pl.ds(a, n)]

    def forward(ch, s):
        return remote(land[ch].at[s], home(core, ch, s), s_fs.at[ch, s], s_fr.at[ch, s], sib)

    def settle(ch, s):
        return pltpu.make_async_copy(land[ch].at[s], home(core, ch, s), s_home.at[ch, s])

    def spill_to(ch):
        return remote(spill[ch], spill_in[ch], s_os.at[ch], s_or.at[ch], side)

    def hand_over(ch):
        return remote(land[ch].at[n_slots - 1], extra[ch], s_xs.at[ch], s_xr.at[ch], side)

    def forward_extra(ch):
        return remote(extra[ch], home(core, ch, n_slots), s_fs.at[ch, n_slots], s_fr.at[ch, n_slots], sib)

    def settle_extra(ch):
        return pltpu.make_async_copy(extra[ch], home(core, ch, n_slots), s_home.at[ch, n_slots])

    last = n_slots - 1 if detour else n_slots
    sib_home = []

    def pack(ch):
        kv, a, n = split[ch]
        pk_local[ch].wait()
        sib_pk[ch].wait_recv()
        if detour:
            spill[ch][...] = pks[ch][plan_ref[n_slots]]
        for s in range(last):
            stage[ch][s] = pks[ch][plan_ref[s]]
        if detour:
            spill_to(ch).start()
        sib_home.append(local(pks[ch].at[pl.ds(other * nb, nb)], sib_ref.at[core, kv, :, pl.ds(a, n)], s_sib.at[ch]))

    def pack_last(ch):
        spill_to(ch).wait_recv()
        mine = plan_ref[rows + 2 * nb] >= n_slots
        own = pks[ch][plan_ref[n_slots - 1]]
        stage[ch][n_slots - 1] = jnp.where(mine, own, spill_in[ch][...])

    queue = []

    def send(ch, lo=0, hi=None):
        hi = last if hi is None else min(hi, last)
        for s in range(lo, hi):
            bulk(ch, s).start()
        if lo < hi:
            queue.append((ch, lo, hi))

    def send_last(*chs):
        if detour:
            for ch in chs:
                pack_last(ch)
            for ch in chs:
                bulk(ch, n_slots - 1).start()
                queue.append((ch, n_slots - 1, n_slots))

    def drain(count=None):
        todo = queue[:count]
        del queue[:count]
        for ch, lo, hi in todo:
            @pl.loop(lo, hi)
            def _(s, ch=ch):
                bulk(ch, s).wait_recv()
                forward(ch, s).start()
                settle(ch, s).start()

            if detour and hi == n_slots:
                hand_over(ch).start()

    for ch in range(2):
        pack(ch)
        send(ch)

    payall[0] = pay_ref[...]
    for c in pay_out:
        c.wait_recv()
    for i in range(span):
        resid[pl.ds(pl.multiple_of(i * 8, 8), 8), :] = payall[lax.rem(place - i + span, span)]

    lane = lax.broadcasted_iota(jnp.int32, (1, dm), 1)
    low = lax.rem(lane, hd) < hd // 2
    t = pos_ref[0]
    att_scale = hd ** -0.5
    cosv = cos_ref[...]
    sinv = sin_ref[...]

    def rope(x):
        swapped = jnp.where(low, pltpu.roll(x, dm - hd // 2, 1), pltpu.roll(x, hd // 2, 1))
        return x * cosv + swapped * sinv

    ffp = wg_ref.shape[2] // FF_PARTS
    qw = 256
    hq = qw // hd
    n_quad = dm // qw
    lane_q = lax.broadcasted_iota(jnp.int32, (1, qw), 1)
    head_mask = [lax.div(lane_q, hd) == h for h in range(hq)]
    low_q = lax.rem(lane_q, hd) < hd // 2
    slot_id = seq * slots + lax.broadcasted_iota(jnp.int32, (1, slots), 1)
    valid = slot_id < t
    pm = pm_ref[...]
    pm4 = jnp.concatenate([pm] * hq, axis=0)
    nrow = pm.shape[0]

    for l in range(n_layers):
        hidden = rms(resid[...], ga_ref[l:l + 1, :])
        for i in range(3):
            weights[l, i].wait()
        q = jnp.dot(hidden, b_q[l], preferred_element_type=F32).astype(BF16).astype(F32)
        k = jnp.dot(hidden, b_k[l], preferred_element_type=F32).astype(BF16).astype(F32)
        v = jnp.dot(hidden, b_v[l], preferred_element_type=F32).astype(BF16).astype(F32)
        q = rope(q).astype(BF16).astype(F32)
        k = rope(k).astype(BF16).astype(F32)
        qbuf[...] = q
        knew[...] = k
        vnew[...] = v
        mine = pl.ds(pl.multiple_of(place * 8, 8), 8)
        new_ref[l, 0] = knew[mine, :]
        new_ref[l, 1] = vnew[mine, :]
        if l == 0:
            for ch in range(2, n_ch):
                pack(ch)
            send(2, 0, EARLY)
            for i in range(n_ch):
                att[1, i].wait()
            load_weights(0, range(3, 7))
            load_weights(1, range(0, 3))
            load_weights(1, range(3, 7))
            for i in range(n_vbuf):
                voc_copy(i, i).start()
        @pl.loop(0, n_quad)
        def _(g, l=l):
            gs = pl.ds(pl.multiple_of(g * qw, qw), qw)
            qg = qbuf[:, gs]
            qq = jnp.concatenate([jnp.where(hm, qg, 0.0) for hm in head_mask], axis=0).astype(BF16)
            s = jnp.zeros((hq * nrow, slots), F32)
            for c in range(nb):
                sc = jnp.dot(qq, kv_att[l, 0, c, gs], preferred_element_type=F32)
                s = jnp.where(pm4 == place * 8 + c, sc, s)
            s = jnp.where(valid, s * att_scale, NEG)
            m = jnp.max(s, axis=-1, keepdims=True)
            e = jnp.where(valid, jnp.exp(s - m), 0.0)
            den = jnp.sum(e, axis=-1, keepdims=True)
            acc = jnp.zeros((hq * nrow, qw), F32)
            for c in range(nb):
                ec = jnp.where(pm4 == place * 8 + c, e, 0.0).astype(BF16)
                acc = acc + lax.dot_general(ec, kv_att[l, 1, c, gs], (((1,), (1,)), ((), ())),
                                            preferred_element_type=F32)

            def fold(x):
                y = jnp.zeros((nrow, qw), F32)
                for h in range(hq):
                    y = jnp.where(head_mask[h], x[h * nrow:(h + 1) * nrow], y)
                return y

            for j, x in enumerate((fold(acc), jnp.where(low_q, fold(m), fold(den)))):
                for w in range(qw // 128):
                    pbuf[l, g * (qw // 128) + w, j] = x[:, w * 128:(w + 1) * 128]
        ex1 = []
        for dj in range(1, sp_n):
            c = remote(pbuf.at[l, lax.rem(seq + dj, sp_n)], rbuf.at[l, dj], s_1s.at[l, dj], s_1r.at[l, dj], peer(0, dj))
            c.start()
            ex1.append(c)
        rbuf[l, 0] = pbuf[l, seq]
        js = pl.ds(pl.multiple_of(seq * 128, 128), 128)
        prod = qbuf[:, js] * knew[:, js]
        lane2 = lax.broadcasted_iota(jnp.int32, (1, 128), 1)
        s_new = jnp.zeros((nrow, 128), F32)
        for h in range(128 // hd):
            hm = lax.div(lane2, hd) == h
            s_new = jnp.where(hm, jnp.sum(jnp.where(hm, prod, 0.0), axis=-1, keepdims=True), s_new)
        s_new = s_new * att_scale
        for c in ex1:
            c.wait_recv()
        low2 = lax.rem(lane2, hd) < hd // 2
        ml = [rbuf[l, dj, 1] for dj in range(sp_n)]
        maxes = [jnp.where(low2, x, pltpu.roll(x, hd // 2, 1)) for x in ml]
        sums = [jnp.where(low2, pltpu.roll(x, 128 - hd // 2, 1), x) for x in ml]
        m_all = s_new
        for x in maxes:
            m_all = jnp.maximum(m_all, x)
        w_new = jnp.exp(s_new - m_all)
        num = w_new * vnew[:, js]
        den = w_new
        for dj in range(sp_n):
            wj = jnp.exp(maxes[dj] - m_all)
            num = num + wj * rbuf[l, dj, 0]
            den = den + wj * sums[dj]
        o = jnp.where(lax.div(pm[:, 0:128], 8) == place, num / den, 0.0).astype(BF16)
        abuf[l] = o
        ex2 = []
        for n, (di, dj) in enumerate(everyone):
            c = remote(abuf.at[l], gbuf.at[l, n + 1], s_2s.at[l, n], s_2r.at[l, n], peer(di, dj))
            c.start()
            ex2.append(c)
        if l == 0:
            send_last(0, 1, 2)
            send(2, EARLY)
        else:
            send_last(3, 4)
            send(3)
            send(4)
        if l == 1:
            drain(2)
        gbuf[l, 0] = o
        for i in range(3, 7):
            weights[l, i].wait()
        for c in ex2:
            c.wait_recv()
        for dj in range(sp_n):
            total = gbuf[l, dj].astype(F32)
            for di in range(1, span):
                total = total + gbuf[l, di * sp_n + dj].astype(F32)
            off = pl.multiple_of(lax.rem(seq - dj + sp_n, sp_n) * 128, 128)
            attn[:, pl.ds(off, 128)] = total
        r = resid[...]
        r = r + jnp.dot(attn[...].astype(BF16), b_o[l], preferred_element_type=F32).astype(BF16).astype(F32)
        hidden = rms(r, gm_ref[l:l + 1, :])
        attn[...] = jnp.zeros_like(attn)

        @pl.loop(0, FF_PARTS)
        def _(f, l=l, hidden=hidden):
            fs = pl.ds(pl.multiple_of(f * ffp, ffp), ffp)
            gate = jnp.dot(hidden, b_g[l, :, fs], preferred_element_type=F32).astype(BF16).astype(F32)
            up = jnp.dot(hidden, b_u[l, :, fs], preferred_element_type=F32).astype(BF16).astype(F32)
            act = (gate * jax.nn.sigmoid(gate) * up).astype(BF16)
            attn[...] += jnp.dot(act, b_d[l, fs], preferred_element_type=F32)

        r = r + attn[...].astype(BF16).astype(F32)
        resid[...] = r
        for c in ex1 + ex2:
            c.wait_send()

    new_home = local(new_ref, new_out, s_out.at[0])
    drain(max(0, len(queue) - (4 if detour else 2)))
    own = resid[pl.ds(pl.multiple_of(place * 8, 8), 8), :]
    hv = rms(own, gf_ref[...].astype(F32).reshape(1, dm))

    @pl.loop(0, n_full)
    def _(i):
        slot = lax.rem(i, n_vbuf)
        voc_copy(i, slot).wait()
        cand_ref[:, pl.ds(pl.multiple_of(i * CHUNK, CHUNK), CHUNK)] = jnp.dot(
            hv, vbuf[slot], preferred_element_type=F32)

        @pl.when(i + n_vbuf < n_full)
        def _():
            voc_copy(i + n_vbuf, slot).start()

        if tail:
            @pl.when(i + n_vbuf == n_full)
            def _():
                voc_tail().start()

    if tail:
        voc_tail().wait()
        cand_ref[:, pl.ds(n_full * CHUNK, tail)] = jnp.dot(
            hv, vbuf[n_full % n_vbuf, :, pl.ds(0, tail)], preferred_element_type=F32)

    lg = cand_ref[...]
    mx = jnp.max(lg, axis=-1, keepdims=True)
    lse = jnp.log(jnp.sum(jnp.exp(lg - mx), axis=-1, keepdims=True))
    code = pm_ref[pl.ds(pl.multiple_of(place * 8, 8), 8), 0:128]
    lane1 = lax.broadcasted_iota(jnp.int32, (1, 128), 1)
    score = jnp.zeros((8, 1), F32)
    for i in range(span):
        dev = lax.rem(place - i + span, span)
        srow = payall[i, nb:nb + 1, 0:128]
        score = score + jnp.sum(jnp.where(code == dev * 8 + lane1, srow, 0.0), axis=-1, keepdims=True)
    cand_ref[...] = score + ((cand_ref[...] - mx) - lse)

    cand_home = local(cand_ref, cand_out, s_out.at[1])

    def finish(ch):
        @pl.loop(0, n_slots)
        def _(s):
            bulk(ch, s).wait_send()
            settle(ch, s).wait()
            forward(ch, s).wait_send()
            remote(land[ch].at[s], home(other, ch, s), s_fs.at[ch, s], s_fr.at[ch, s], sib).wait_recv()
        if detour:
            spill_to(ch).wait_send()
            hand_over(ch).wait_send()
            settle_extra(ch).wait()
            forward_extra(ch).wait_send()
            remote(extra[ch], home(other, ch, n_slots), s_fs.at[ch, n_slots], s_fr.at[ch, n_slots], sib).wait_recv()

    drain(len(queue) - 1)
    if detour:
        for ch in range(n_ch):
            hand_over(ch).wait_recv()
            forward_extra(ch).start()
            settle_extra(ch).start()
    for c in pay_out + sib_pk + sib_rest:
        c.wait_send()
    for c in sib_rest:
        c.wait_recv()
    for c in sib_home + [new_home, cand_home]:
        c.wait()
    for ch in range(n_ch - 1):
        finish(ch)
    drain()
    finish(n_ch - 1)


def assemble_kernel(dims, plan_ref, pos_ref, new_ref, cand8_ref, k_ref, v_ref, sib_ref, recv_ref,
                    ko_ref, vo_ref, cand_ref, buf, cbuf, c6, nbuf, s_in, s_out, s_c):
    nb = dims[0]
    rows = CORES * nb
    n_layers = k_ref.shape[0]
    slots = k_ref.shape[3]
    seq = lax.axis_index('sp')
    at = pos_ref[0] - seq * slots
    owns = (at >= 0) & (at < slots)
    new_in = pltpu.make_async_copy(new_ref, nbuf, s_c.at[0])
    new_in.start()
    order = [(l, i, b) for l in range(n_layers) for i in range(2) for b in range(nb)]
    for u, (l, i, b) in enumerate(order):
        kind = plan_ref[rows + b]
        idx = plan_ref[rows + nb + b]
        src = (k_ref, v_ref)[i]

        @pl.when(kind == 0)
        def _():
            pltpu.make_async_copy(src.at[l, idx], buf.at[u], s_in.at[u]).start()

        @pl.when(kind == 1)
        def _():
            pltpu.make_async_copy(sib_ref.at[l, i, idx], buf.at[u], s_in.at[u]).start()

        @pl.when(kind == 2)
        def _():
            pltpu.make_async_copy(recv_ref.at[l, i, idx], buf.at[u], s_in.at[u]).start()

    cand_in = pltpu.make_async_copy(cand8_ref, cbuf, s_c.at[1])
    cand_in.start()
    new_in.wait()
    tile = jnp.clip(lax.div(at, 128), 0, slots // 128 - 1)
    lane = lax.broadcasted_iota(jnp.int32, (1, 128), 1)
    outs = []
    for l in range(n_layers):
        for i in range(2):
            cols = jnp.transpose(nbuf[l, i])
            for b in range(nb):
                u = (l * 2 + i) * nb + b
                pltpu.make_async_copy((k_ref, v_ref)[i].at[l, b], buf.at[u], s_in.at[u]).wait()

                @pl.when(owns)
                def _():
                    ts = pl.ds(pl.multiple_of(tile * 128, 128), 128)
                    old = buf[u, :, ts]
                    buf[u, :, ts] = jnp.where(lane == at - tile * 128, cols[:, b:b + 1].astype(BF16), old)

                c = pltpu.make_async_copy(buf.at[u], (ko_ref, vo_ref)[i].at[l, b], s_out.at[u])
                c.start()
                outs.append(c)
    cand_in.wait()
    c6[...] = cbuf[0:nb, :]
    cand_back = pltpu.make_async_copy(c6, cand_ref, s_c.at[2])
    cand_back.start()
    for c in outs + [cand_back]:
        c.wait()


def solution(mesh):
    beam_spec = P(('dp', 'beam'))
    row_spec = P(('dp', 'beam'), None)
    cache_spec = P(None, ('dp', 'beam'), 'sp', None, None)
    rep = P()
    sp_n = mesh.shape['sp']

    def local_step(tok_emb, parent, position, beam_score, k_cache, v_cache, w_query, w_key, w_value, w_out,
                   w_gate, w_up, w_down, g_attn, g_mlp, g_final, w_vocab):
        n_layers, nb, slots, heads, hd = k_cache.shape
        width = parent.shape[1]
        span = width // nb
        dm = tok_emb.shape[1]
        ff = w_gate.shape[2]
        vocab = w_vocab.shape[1]
        rows = CORES * nb
        hrow = heads * hd
        kt = k_cache.transpose(0, 1, 3, 4, 2).reshape(n_layers, nb, hrow, slots)
        vt = v_cache.transpose(0, 1, 3, 4, 2).reshape(n_layers, nb, hrow, slots)
        smem = pl.BlockSpec(memory_space=pltpu.SMEM)
        vmem = pl.BlockSpec(memory_space=pltpu.VMEM)
        hbm = pl.BlockSpec(memory_space=pl.ANY)
        sds = jax.ShapeDtypeStruct

        levels = [n for n in LEVELS if n < rows] + [rows]
        n_chips = mesh.shape['beam'] // CORES
        detour = parent.shape[0] == 2 and span == 2 * CORES and n_chips == 4
        plan, branch, pay, pm = pl.pallas_call(
            functools.partial(plan_kernel, (nb, span), levels, detour),
            out_shape=(sds((64,), jnp.int32), sds((1,), jnp.int32), sds((8, dm), F32), sds((8 * span, slots), jnp.int32)),
            in_specs=[smem, smem, vmem], out_specs=(smem, smem, vmem, vmem),
            scratch_shapes=[pltpu.SMEM((rows,), jnp.int32)],
            name='plan',
        )(parent, beam_score, tok_emb)

        half_dim = hd // 2
        lane = lax.broadcasted_iota(jnp.int32, (1, hrow), 1)
        inv_freq = ROPE_BASE ** (-2.0 * (lane % half_dim).astype(F32) / hd)
        angles = position[0].astype(F32) * inv_freq
        cos_t = jnp.cos(angles)
        sin_t = jnp.where(lane % hd < half_dim, -1.0, 1.0) * jnp.sin(angles)

        def main(n_slots, cid, *ops):
            np_ = dm // 128
            nrow = 8 * span
            dma = pltpu.SemaphoreType.DMA
            n_vbuf = VBUF if 2 * n_slots <= rows else VBUF // 2
            sizes = [hrow // of * n for _, _, n, of in SPLIT]
            nch = len(sizes)
            scratch = [
                [pltpu.VMEM((rows, n, slots), BF16) for n in sizes],
                [pltpu.VMEM((n_slots, n, slots), BF16) for n in sizes],
                [pltpu.VMEM((n_slots, n, slots), BF16) for n in sizes],
                [pltpu.VMEM((n, slots), BF16) for n in sizes],
                [pltpu.VMEM((n, slots), BF16) for n in sizes],
                [pltpu.VMEM((n, slots), BF16) for n in sizes],
                pltpu.VMEM((8, vocab), F32), pltpu.VMEM((n_layers, 2, 8, hrow), F32),
                pltpu.VMEM((n_layers, 2, nb, hrow, slots), BF16),
                pltpu.VMEM((n_layers, dm, hrow), BF16),
                pltpu.VMEM((n_layers, dm, hrow), BF16),
                pltpu.VMEM((n_layers, dm, hrow), BF16),
                pltpu.VMEM((n_layers, hrow, dm), BF16),
                pltpu.VMEM((n_layers, dm, ff), BF16),
                pltpu.VMEM((n_layers, dm, ff), BF16),
                pltpu.VMEM((n_layers, ff, dm), BF16),
                pltpu.VMEM((n_vbuf, dm, CHUNK), BF16),
                pltpu.VMEM((span, 8, dm), F32),
                pltpu.VMEM((nrow, dm), F32),
                pltpu.VMEM((nrow, dm), F32),
                pltpu.VMEM((nrow, dm), F32),
                pltpu.VMEM((nrow, dm), F32),
                pltpu.VMEM((n_layers, np_, 2, nrow, 128), F32),
                pltpu.VMEM((n_layers, sp_n, 2, nrow, 128), F32),
                pltpu.VMEM((n_layers, nrow, 128), BF16),
                pltpu.VMEM((n_layers, span * sp_n, nrow, 128), BF16),
                pltpu.VMEM((nrow, dm), F32),
                dma((span,)), dma((span,)),
                dma((nch,)), dma((nch,)), dma((nch,)), dma((nch,)), dma((2,)), dma((2,)),
                dma((nch, n_slots)), dma((nch, n_slots)), dma((nch, n_slots + 1)), dma((nch, n_slots + 1)),
                dma((nch, n_slots + 1)), dma((nch,)), dma((nch,)), dma((nch,)), dma((nch,)), dma((2,)),
                dma((2, nch)), dma((n_layers, 7)), dma((n_vbuf,)),
                dma((n_layers, sp_n)), dma((n_layers, sp_n)),
                dma((n_layers, span * sp_n)), dma((n_layers, span * sp_n)),
            ]
            return pl.pallas_call(
                functools.partial(main_kernel, (nb, span, sp_n, hd), n_slots, detour and n_slots < rows),
                out_shape=(sds((8, vocab), F32), sds((n_layers, 2, 8, hrow), F32),
                           sds((n_layers, 2, nb, hrow, slots), BF16),
                           sds((n_layers, 2, rows, hrow, slots), BF16)),
                in_specs=[smem, smem] + [vmem] * 7 + [hbm] * 10,
                out_specs=(hbm, hbm, hbm, hbm),
                scratch_shapes=scratch,
                compiler_params=pltpu.CompilerParams(collective_id=cid, has_side_effects=True,
                                                     vmem_limit_bytes=VMEM_LIMIT),
                name=f'main{n_slots}',
            )(*ops)

        ops = (plan, position, pay, pm, cos_t, sin_t, g_attn, g_mlp, g_final, kt, vt,
               w_query, w_key, w_value, w_out, w_gate, w_up, w_down, w_vocab)
        cand8, new, sib, recv = lax.switch(
            branch[0], [functools.partial(main, n, i) for i, n in enumerate(levels)], *ops)

        ko, vo, cand = pl.pallas_call(
            functools.partial(assemble_kernel, (nb,)),
            out_shape=(sds(kt.shape, BF16), sds(vt.shape, BF16), sds((nb, vocab), F32)),
            in_specs=[smem, smem, hbm, hbm, hbm, hbm, hbm, hbm],
            out_specs=(hbm, hbm, hbm),
            scratch_shapes=[pltpu.VMEM((n_layers * 2 * nb, hrow, slots), BF16),
                            pltpu.VMEM((8, vocab), F32), pltpu.VMEM((nb, vocab), F32), pltpu.VMEM((n_layers, 2, 8, hrow), F32),
                            pltpu.SemaphoreType.DMA((n_layers * 2 * nb,)),
                            pltpu.SemaphoreType.DMA((n_layers * 2 * nb,)), pltpu.SemaphoreType.DMA((3,))],
            compiler_params=pltpu.CompilerParams(vmem_limit_bytes=VMEM_LIMIT),
            name='assemble',
        )(plan, position, new, cand8, kt, vt, sib, recv)

        def back(x):
            return x.reshape(n_layers, nb, heads, hd, slots).transpose(0, 1, 4, 2, 3)

        return back(ko), back(vo), cand

    in_specs = (row_spec, P('dp', None), rep, beam_spec, cache_spec, cache_spec) + (rep,) * 11
    return jax.shard_map(local_step, mesh=mesh, in_specs=in_specs, out_specs=(cache_spec, cache_spec, row_spec),
                         check_vma=False)
```

```python
import functools

import jax
import jax.numpy as jnp
from jax import lax
from jax.experimental import pallas as pl
from jax.experimental.pallas import tpu as pltpu
from jax.sharding import PartitionSpec as P

ROPE_BASE = 10000.0
NORM_EPS = 1e-6
NEG = -1e30
CORES = 2
LEVELS = (3, 4, 5, 6)
CHUNK = 2048
VBUF = 10
MID = 4
FF_PARTS = 2
SPLIT = ((0, 0, 1, 8), (0, 1, 3, 8), (0, 4, 4, 8), (1, 0, 4, 8), (1, 4, 4, 8))
EARLY = 1
VMEM_LIMIT = 64 * 1024 * 1024 - 64 * 1024
MESH = pl.DeviceIdType.MESH
F32 = jnp.float32
BF16 = jnp.bfloat16


def rms(x, g):
    ms = jnp.mean(x * x, axis=-1, keepdims=True)
    return (x * lax.rsqrt(ms + NORM_EPS) * g.astype(F32)).astype(BF16)


def plan_kernel(dims, levels, detour, parent_ref, score_ref, tok_ref, plan_ref, branch_ref, pay_ref, pm_ref, rank_ref):
    nb, span = dims
    rows = CORES * nb
    n_sent, width = parent_ref.shape
    me = lax.axis_index('beam')
    sent = me // span
    place = lax.rem(me, span)
    chip = lax.div(place, CORES)

    def needed(s, to_chip):
        base = (1 - to_chip) * rows
        mask = jnp.int32(0)
        for k in range(rows):
            p = parent_ref[s, to_chip * rows + k] - s * width - base
            mask = mask | jnp.where((p >= 0) & (p < rows), jnp.left_shift(jnp.int32(1), jnp.clip(p, 0, rows - 1)), 0)
        return mask

    def bit(mask, p):
        return jnp.right_shift(mask, p) & 1

    count = {(s, tc): sum(bit(needed(s, tc), p) for p in range(rows)) for s in range(n_sent) for tc in range(2)}
    most = functools.reduce(jnp.maximum, count.values())
    share = most
    if detour:
        share = functools.reduce(jnp.maximum, [most - 1] + [
            lax.div(count[0, tc] + count[1, 1 - tc] + 1, 2) for tc in range(2)])
    out_mask = needed(sent, 1 - chip)
    in_mask = needed(sent, chip)
    for p in range(rows + 1):
        plan_ref[p] = 0
    cnt = jnp.int32(0)
    for p in range(rows):
        @pl.when(bit(out_mask, p) == 1)
        def _(p=p, cnt=cnt):
            plan_ref[cnt] = p
        cnt = cnt + bit(out_mask, p)
    cnt = jnp.int32(0)
    for p in range(rows):
        rank_ref[p] = cnt
        cnt = cnt + bit(in_mask, p)
    for b in range(nb):
        par = parent_ref[sent, place * nb + b] - sent * width
        dev = lax.div(par, nb)
        row = lax.rem(par, nb)
        far = lax.div(dev, CORES) != chip
        slot = rank_ref[jnp.clip(par - (1 - chip) * rows, 0, rows - 1)]
        plan_ref[rows + b] = jnp.where(far, 2, jnp.where(dev == place, 0, 1))
        plan_ref[rows + nb + b] = jnp.where(far, slot, row)
    branch_ref[0] = sum((share > n).astype(jnp.int32) for n in levels[:-1])
    plan_ref[rows + 2 * nb] = sum(bit(out_mask, p) for p in range(rows))
    for i in range(span):
        for b in range(8):
            if b < nb:
                par = parent_ref[sent, i * nb + b] - sent * width
                code = lax.div(par, nb) * 8 + lax.rem(par, nb)
            else:
                code = jnp.int32(-1)
            pm_ref[i * 8 + b:i * 8 + b + 1, :] = jnp.full((1, pm_ref.shape[1]), code, jnp.int32)
    lane = lax.broadcasted_iota(jnp.int32, (1, pay_ref.shape[1]), 1)
    row = jnp.zeros((1, pay_ref.shape[1]), F32)
    for b in range(nb):
        row = jnp.where(lane == b, score_ref[b], row)
    pay_ref[0:nb, :] = tok_ref[...].astype(F32)
    pay_ref[nb:nb + 1, :] = row
    pay_ref[nb + 1:8, :] = jnp.zeros((8 - nb - 1, pay_ref.shape[1]), F32)


def main_kernel(dims, n_slots, detour, plan_ref, pos_ref, pay_ref, pm_ref, cos_ref, sin_ref, ga_ref, gm_ref, gf_ref,
                k_ref, v_ref, wq_ref, wk_ref, wv_ref, wo_ref, wg_ref, wu_ref, wd_ref, wvoc_ref,
                cand_out, new_out, sib_ref, recv_ref, pks, stage, land, spill, spill_in, extra, cand_ref, new_ref, kv_att, b_q, b_k, b_v, b_o, b_g, b_u, b_d, vbuf,
                payall, resid, qbuf, knew, vnew, pbuf, rbuf, abuf, gbuf, attn,
                s_pl, s_pr, s_pkl, s_pks, s_pkr, s_sib, s_ss, s_sr, s_bs, s_br, s_fs, s_fr, s_home, s_os, s_or, s_xs, s_xr, s_out,
                s_att, s_w, s_voc, s_1s, s_1r, s_2s, s_2r):
    nb, span, sp_n, hd = dims
    n_layers = ga_ref.shape[0]
    dm = ga_ref.shape[1]
    slots = k_ref.shape[3]
    hrow = k_ref.shape[2]
    n_vbuf = vbuf.shape[0]
    split = [(kv, hrow // of * a, hrow // of * n) for kv, a, n, of in SPLIT]
    n_ch = len(split)
    seq = lax.axis_index('sp')
    me = lax.axis_index('beam')
    place = lax.rem(me, span)
    base = me - place
    core = lax.rem(me, CORES)
    other = 1 - core
    rows = CORES * nb
    sib = {'beam': base + lax.div(place, CORES) * CORES + other}
    par = {'beam': base + lax.rem(place + CORES, span)}
    chip = lax.div(me, CORES)
    side = {'beam': (span - 1 - chip) * CORES + core}

    def peer(di, dj):
        return {'beam': base + lax.rem(place + di, span), 'sp': lax.rem(seq + dj, sp_n)}

    everyone = [(di, dj) for di in range(span) for dj in range(sp_n) if (di, dj) != (0, 0)]

    barrier = pltpu.get_barrier_semaphore()
    for di, dj in everyone:
        pl.semaphore_signal(barrier, inc=1, device_id=peer(di, dj), device_id_type=MESH)
    if detour:
        pl.semaphore_signal(barrier, inc=1, device_id=side, device_id_type=MESH)

    def local(src, dst, sem):
        c = pltpu.make_async_copy(src, dst, sem)
        c.start()
        return c

    def remote(src, dst, ss, rs, dev):
        return pltpu.make_async_remote_copy(src_ref=src, dst_ref=dst, send_sem=ss, recv_sem=rs,
                                            device_id=dev, device_id_type=MESH)

    src_of = (k_ref, v_ref)
    att, pk_local = {}, []

    def load_cache(role, lay, i):
        kv, a, n = split[i]
        att[role, i] = local(src_of[kv].at[lay, :, pl.ds(a, n)], kv_att.at[lay, kv, :, pl.ds(a, n)], s_att.at[role, i])

    for i, (kv, a, n) in enumerate(split):
        load_cache(0, other, i)
        pk_local.append(local(src_of[kv].at[core, :, pl.ds(a, n)], pks[i].at[pl.ds(core * nb, nb)], s_pkl.at[i]))
    w0 = [local(src.at[0], dst.at[0], s_w.at[0, i])
          for i, (src, dst) in enumerate(((wq_ref, b_q), (wk_ref, b_k), (wv_ref, b_v)))]
    for i in range(n_ch):
        load_cache(1, core, i)
    weights = {(0, i): c for i, c in enumerate(w0)}
    pairs = ((wq_ref, b_q), (wk_ref, b_k), (wv_ref, b_v), (wo_ref, b_o), (wg_ref, b_g), (wu_ref, b_u), (wd_ref, b_d))

    def load_weights(l, which):
        for i in which:
            weights[l, i] = local(pairs[i][0].at[l], pairs[i][1].at[l], s_w.at[l, i])

    vocab = wvoc_ref.shape[1]
    n_full = vocab // CHUNK
    tail = vocab - n_full * CHUNK
    n_mid = n_full * MID // 8

    def voc_copy(i, slot):
        return pltpu.make_async_copy(wvoc_ref.at[:, pl.ds(i * CHUNK, CHUNK)], vbuf.at[slot], s_voc.at[slot])

    def voc_tail():
        return pltpu.make_async_copy(wvoc_ref.at[:, pl.ds(n_full * CHUNK, tail)],
                                     vbuf.at[n_full % n_vbuf, :, pl.ds(0, tail)], s_voc.at[n_full % n_vbuf])

    pl.semaphore_wait(barrier, len(everyone) + int(detour))

    pay_out = []
    for di in range(1, span):
        c = remote(pay_ref, payall.at[di], s_pl.at[di], s_pr.at[di], peer(di, 0))
        c.start()
        pay_out.append(c)
    sib_pk = []
    for i, (kv, a, n) in enumerate(split):
        att[0, i].wait()
        c = remote(kv_att.at[other, kv, :, pl.ds(a, n)], pks[i].at[pl.ds(core * nb, nb)], s_pks.at[i], s_pkr.at[i], sib)
        c.start()
        sib_pk.append(c)
    sib_rest = []
    for i, src in enumerate((k_ref, v_ref)):
        c = remote(src.at[core], sib_ref.at[core, i], s_ss.at[i], s_sr.at[i], sib)
        c.start()
        sib_rest.append(c)

    def bulk(ch, s):
        return remote(stage[ch].at[s], land[ch].at[s], s_bs.at[ch, s], s_br.at[ch, s], par)

    def home(lay, ch, s):
        kv, a, n = split[ch]
        return recv_ref.at[lay, kv, s, pl.ds(a, n)]

    def forward(ch, s):
        return remote(land[ch].at[s], home(core, ch, s), s_fs.at[ch, s], s_fr.at[ch, s], sib)

    def settle(ch, s):
        return pltpu.make_async_copy(land[ch].at[s], home(core, ch, s), s_home.at[ch, s])

    def spill_to(ch):
        return remote(spill[ch], spill_in[ch], s_os.at[ch], s_or.at[ch], side)

    def hand_over(ch):
        return remote(land[ch].at[n_slots - 1], extra[ch], s_xs.at[ch], s_xr.at[ch], side)

    def forward_extra(ch):
        return remote(extra[ch], home(core, ch, n_slots), s_fs.at[ch, n_slots], s_fr.at[ch, n_slots], sib)

    def settle_extra(ch):
        return pltpu.make_async_copy(extra[ch], home(core, ch, n_slots), s_home.at[ch, n_slots])

    last = n_slots - 1 if detour else n_slots
    sib_home = []

    def pack(ch):
        kv, a, n = split[ch]
        pk_local[ch].wait()
        sib_pk[ch].wait_recv()
        if detour:
            spill[ch][...] = pks[ch][plan_ref[n_slots]]
        for s in range(last):
            stage[ch][s] = pks[ch][plan_ref[s]]
        if detour:
            spill_to(ch).start()
        sib_home.append(local(pks[ch].at[pl.ds(other * nb, nb)], sib_ref.at[core, kv, :, pl.ds(a, n)], s_sib.at[ch]))

    def pack_last(ch):
        spill_to(ch).wait_recv()
        mine = plan_ref[rows + 2 * nb] >= n_slots
        own = pks[ch][plan_ref[n_slots - 1]]
        stage[ch][n_slots - 1] = jnp.where(mine, own, spill_in[ch][...])

    queue = []

    def send(ch, lo=0, hi=None):
        hi = last if hi is None else min(hi, last)
        for s in range(lo, hi):
            bulk(ch, s).start()
        if lo < hi:
            queue.append((ch, lo, hi))

    def send_last(*chs):
        if detour:
            for ch in chs:
                pack_last(ch)
            for ch in chs:
                bulk(ch, n_slots - 1).start()
                queue.append((ch, n_slots - 1, n_slots))

    def drain(count=None):
        todo = queue[:count]
        del queue[:count]
        for ch, lo, hi in todo:
            @pl.loop(lo, hi)
            def _(s, ch=ch):
                bulk(ch, s).wait_recv()
                forward(ch, s).start()
                settle(ch, s).start()

            if detour and hi == n_slots:
                hand_over(ch).start()

    for ch in range(2):
        pack(ch)
        send(ch)

    payall[0] = pay_ref[...]
    for c in pay_out:
        c.wait_recv()
    for i in range(span):
        resid[pl.ds(pl.multiple_of(i * 8, 8), 8), :] = payall[lax.rem(place - i + span, span)]

    lane = lax.broadcasted_iota(jnp.int32, (1, dm), 1)
    low = lax.rem(lane, hd) < hd // 2
    t = pos_ref[0]
    att_scale = hd ** -0.5
    cosv = cos_ref[...]
    sinv = sin_ref[...]

    def rope(x):
        swapped = jnp.where(low, pltpu.roll(x, dm - hd // 2, 1), pltpu.roll(x, hd // 2, 1))
        return x * cosv + swapped * sinv

    ffp = wg_ref.shape[2] // FF_PARTS
    qw = 256
    hq = qw // hd
    n_quad = dm // qw
    lane_q = lax.broadcasted_iota(jnp.int32, (1, qw), 1)
    head_mask = [lax.div(lane_q, hd) == h for h in range(hq)]
    low_q = lax.rem(lane_q, hd) < hd // 2
    slot_id = seq * slots + lax.broadcasted_iota(jnp.int32, (1, slots), 1)
    valid = slot_id < t
    pm = pm_ref[...]
    pm4 = jnp.concatenate([pm] * hq, axis=0)
    nrow = pm.shape[0]

    for l in range(n_layers):
        hidden = rms(resid[...], ga_ref[l:l + 1, :])
        for i in range(3):
            weights[l, i].wait()
        q = jnp.dot(hidden, b_q[l], preferred_element_type=F32).astype(BF16).astype(F32)
        k = jnp.dot(hidden, b_k[l], preferred_element_type=F32).astype(BF16).astype(F32)
        v = jnp.dot(hidden, b_v[l], preferred_element_type=F32).astype(BF16).astype(F32)
        q = rope(q).astype(BF16).astype(F32)
        k = rope(k).astype(BF16).astype(F32)
        qbuf[...] = q
        knew[...] = k
        vnew[...] = v
        mine = pl.ds(pl.multiple_of(place * 8, 8), 8)
        new_ref[l, 0] = knew[mine, :]
        new_ref[l, 1] = vnew[mine, :]
        if l == 0:
            for ch in range(2, n_ch):
                pack(ch)
            send(2, 0, EARLY)
            for i in range(n_ch):
                att[1, i].wait()
            load_weights(0, range(3, 7))
            load_weights(1, range(0, 3))
            load_weights(1, range(3, 7))
            for i in range(n_vbuf):
                voc_copy(i, i).start()
        @pl.loop(0, n_quad)
        def _(g, l=l):
            gs = pl.ds(pl.multiple_of(g * qw, qw), qw)
            qg = qbuf[:, gs]
            qq = jnp.concatenate([jnp.where(hm, qg, 0.0) for hm in head_mask], axis=0).astype(BF16)
            s = jnp.zeros((hq * nrow, slots), F32)
            for c in range(nb):
                sc = jnp.dot(qq, kv_att[l, 0, c, gs], preferred_element_type=F32)
                s = jnp.where(pm4 == place * 8 + c, sc, s)
            s = jnp.where(valid, s * att_scale, NEG)
            m = jnp.max(s, axis=-1, keepdims=True)
            e = jnp.where(valid, jnp.exp(s - m), 0.0)
            den = jnp.sum(e, axis=-1, keepdims=True)
            acc = jnp.zeros((hq * nrow, qw), F32)
            for c in range(nb):
                ec = jnp.where(pm4 == place * 8 + c, e, 0.0).astype(BF16)
                acc = acc + lax.dot_general(ec, kv_att[l, 1, c, gs], (((1,), (1,)), ((), ())),
                                            preferred_element_type=F32)

            def fold(x):
                y = jnp.zeros((nrow, qw), F32)
                for h in range(hq):
                    y = jnp.where(head_mask[h], x[h * nrow:(h + 1) * nrow], y)
                return y

            for j, x in enumerate((fold(acc), jnp.where(low_q, fold(m), fold(den)))):
                for w in range(qw // 128):
                    pbuf[l, g * (qw // 128) + w, j] = x[:, w * 128:(w + 1) * 128]
        ex1 = []
        for dj in range(1, sp_n):
            c = remote(pbuf.at[l, lax.rem(seq + dj, sp_n)], rbuf.at[l, dj], s_1s.at[l, dj], s_1r.at[l, dj], peer(0, dj))
            c.start()
            ex1.append(c)
        rbuf[l, 0] = pbuf[l, seq]
        js = pl.ds(pl.multiple_of(seq * 128, 128), 128)
        prod = qbuf[:, js] * knew[:, js]
        lane2 = lax.broadcasted_iota(jnp.int32, (1, 128), 1)
        s_new = jnp.zeros((nrow, 128), F32)
        for h in range(128 // hd):
            hm = lax.div(lane2, hd) == h
            s_new = jnp.where(hm, jnp.sum(jnp.where(hm, prod, 0.0), axis=-1, keepdims=True), s_new)
        s_new = s_new * att_scale
        for c in ex1:
            c.wait_recv()
        low2 = lax.rem(lane2, hd) < hd // 2
        ml = [rbuf[l, dj, 1] for dj in range(sp_n)]
        maxes = [jnp.where(low2, x, pltpu.roll(x, hd // 2, 1)) for x in ml]
        sums = [jnp.where(low2, pltpu.roll(x, 128 - hd // 2, 1), x) for x in ml]
        m_all = s_new
        for x in maxes:
            m_all = jnp.maximum(m_all, x)
        w_new = jnp.exp(s_new - m_all)
        num = w_new * vnew[:, js]
        den = w_new
        for dj in range(sp_n):
            wj = jnp.exp(maxes[dj] - m_all)
            num = num + wj * rbuf[l, dj, 0]
            den = den + wj * sums[dj]
        o = jnp.where(lax.div(pm[:, 0:128], 8) == place, num / den, 0.0).astype(BF16)
        abuf[l] = o
        ex2 = []
        for n, (di, dj) in enumerate(everyone):
            c = remote(abuf.at[l], gbuf.at[l, n + 1], s_2s.at[l, n], s_2r.at[l, n], peer(di, dj))
            c.start()
            ex2.append(c)
        if l == 0:
            send_last(0, 1, 2)
            send(2, EARLY)
        else:
            send_last(3, 4)
            send(3)
            send(4)
        if l == 1:
            drain(2)
        gbuf[l, 0] = o
        for i in range(3, 7):
            weights[l, i].wait()
        for c in ex2:
            c.wait_recv()
        for dj in range(sp_n):
            total = gbuf[l, dj].astype(F32)
            for di in range(1, span):
                total = total + gbuf[l, di * sp_n + dj].astype(F32)
            off = pl.multiple_of(lax.rem(seq - dj + sp_n, sp_n) * 128, 128)
            attn[:, pl.ds(off, 128)] = total
        r = resid[...]
        r = r + jnp.dot(attn[...].astype(BF16), b_o[l], preferred_element_type=F32).astype(BF16).astype(F32)
        hidden = rms(r, gm_ref[l:l + 1, :])
        attn[...] = jnp.zeros_like(attn)

        @pl.loop(0, FF_PARTS)
        def _(f, l=l, hidden=hidden):
            fs = pl.ds(pl.multiple_of(f * ffp, ffp), ffp)
            gate = jnp.dot(hidden, b_g[l, :, fs], preferred_element_type=F32).astype(BF16).astype(F32)
            up = jnp.dot(hidden, b_u[l, :, fs], preferred_element_type=F32).astype(BF16).astype(F32)
            act = (gate * jax.nn.sigmoid(gate) * up).astype(BF16)
            attn[...] += jnp.dot(act, b_d[l, fs], preferred_element_type=F32)

        r = r + attn[...].astype(BF16).astype(F32)
        resid[...] = r
        for c in ex1 + ex2:
            c.wait_send()

    new_home = local(new_ref, new_out, s_out.at[0])
    drain(max(0, len(queue) - (4 if detour else 2)))
    own = resid[pl.ds(pl.multiple_of(place * 8, 8), 8), :]
    hv = rms(own, gf_ref[...].astype(F32).reshape(1, dm))

    def voc_step(i):
        slot = lax.rem(i, n_vbuf)
        voc_copy(i, slot).wait()
        cand_ref[:, pl.ds(pl.multiple_of(i * CHUNK, CHUNK), CHUNK)] = jnp.dot(
            hv, vbuf[slot], preferred_element_type=F32)

        @pl.when(i + n_vbuf < n_full)
        def _():
            voc_copy(i + n_vbuf, slot).start()

        if tail:
            @pl.when(i + n_vbuf == n_full)
            def _():
                voc_tail().start()

    pl.loop(0, n_mid)(voc_step)
    if detour:
        drain(2)
    pl.loop(n_mid, n_full)(voc_step)

    if tail:
        voc_tail().wait()
        cand_ref[:, pl.ds(n_full * CHUNK, tail)] = jnp.dot(
            hv, vbuf[n_full % n_vbuf, :, pl.ds(0, tail)], preferred_element_type=F32)

    lg = cand_ref[...]
    mx = jnp.max(lg, axis=-1, keepdims=True)
    lse = jnp.log(jnp.sum(jnp.exp(lg - mx), axis=-1, keepdims=True))
    code = pm_ref[pl.ds(pl.multiple_of(place * 8, 8), 8), 0:128]
    lane1 = lax.broadcasted_iota(jnp.int32, (1, 128), 1)
    score = jnp.zeros((8, 1), F32)
    for i in range(span):
        dev = lax.rem(place - i + span, span)
        srow = payall[i, nb:nb + 1, 0:128]
        score = score + jnp.sum(jnp.where(code == dev * 8 + lane1, srow, 0.0), axis=-1, keepdims=True)
    cand_ref[...] = score + ((cand_ref[...] - mx) - lse)

    cand_home = local(cand_ref, cand_out, s_out.at[1])

    def finish(ch):
        @pl.loop(0, n_slots)
        def _(s):
            bulk(ch, s).wait_send()
            settle(ch, s).wait()
            forward(ch, s).wait_send()
            remote(land[ch].at[s], home(other, ch, s), s_fs.at[ch, s], s_fr.at[ch, s], sib).wait_recv()
        if detour:
            spill_to(ch).wait_send()
            hand_over(ch).wait_send()
            settle_extra(ch).wait()
            forward_extra(ch).wait_send()
            remote(extra[ch], home(other, ch, n_slots), s_fs.at[ch, n_slots], s_fr.at[ch, n_slots], sib).wait_recv()

    drain(len(queue) - 1)
    if detour:
        for ch in range(n_ch):
            hand_over(ch).wait_recv()
            forward_extra(ch).start()
            settle_extra(ch).start()
    for c in pay_out + sib_pk + sib_rest:
        c.wait_send()
    for c in sib_rest:
        c.wait_recv()
    for c in sib_home + [new_home, cand_home]:
        c.wait()
    for ch in range(n_ch - 1):
        finish(ch)
    drain()
    finish(n_ch - 1)


def assemble_kernel(dims, plan_ref, pos_ref, new_ref, cand8_ref, k_ref, v_ref, sib_ref, recv_ref,
                    ko_ref, vo_ref, cand_ref, buf, cbuf, c6, nbuf, s_in, s_out, s_c):
    nb = dims[0]
    rows = CORES * nb
    n_layers = k_ref.shape[0]
    slots = k_ref.shape[3]
    seq = lax.axis_index('sp')
    at = pos_ref[0] - seq * slots
    owns = (at >= 0) & (at < slots)
    new_in = pltpu.make_async_copy(new_ref, nbuf, s_c.at[0])
    new_in.start()
    order = [(l, i, b) for l in range(n_layers) for i in range(2) for b in range(nb)]
    for u, (l, i, b) in enumerate(order):
        kind = plan_ref[rows + b]
        idx = plan_ref[rows + nb + b]
        src = (k_ref, v_ref)[i]

        @pl.when(kind == 0)
        def _():
            pltpu.make_async_copy(src.at[l, idx], buf.at[u], s_in.at[u]).start()

        @pl.when(kind == 1)
        def _():
            pltpu.make_async_copy(sib_ref.at[l, i, idx], buf.at[u], s_in.at[u]).start()

        @pl.when(kind == 2)
        def _():
            pltpu.make_async_copy(recv_ref.at[l, i, idx], buf.at[u], s_in.at[u]).start()

    cand_in = pltpu.make_async_copy(cand8_ref, cbuf, s_c.at[1])
    cand_in.start()
    new_in.wait()
    tile = jnp.clip(lax.div(at, 128), 0, slots // 128 - 1)
    lane = lax.broadcasted_iota(jnp.int32, (1, 128), 1)
    outs = []
    for l in range(n_layers):
        for i in range(2):
            cols = jnp.transpose(nbuf[l, i])
            for b in range(nb):
                u = (l * 2 + i) * nb + b
                pltpu.make_async_copy((k_ref, v_ref)[i].at[l, b], buf.at[u], s_in.at[u]).wait()

                @pl.when(owns)
                def _():
                    ts = pl.ds(pl.multiple_of(tile * 128, 128), 128)
                    old = buf[u, :, ts]
                    buf[u, :, ts] = jnp.where(lane == at - tile * 128, cols[:, b:b + 1].astype(BF16), old)

                c = pltpu.make_async_copy(buf.at[u], (ko_ref, vo_ref)[i].at[l, b], s_out.at[u])
                c.start()
                outs.append(c)
    cand_in.wait()
    c6[...] = cbuf[0:nb, :]
    cand_back = pltpu.make_async_copy(c6, cand_ref, s_c.at[2])
    cand_back.start()
    for c in outs + [cand_back]:
        c.wait()


def solution(mesh):
    beam_spec = P(('dp', 'beam'))
    row_spec = P(('dp', 'beam'), None)
    cache_spec = P(None, ('dp', 'beam'), 'sp', None, None)
    rep = P()
    sp_n = mesh.shape['sp']

    def local_step(tok_emb, parent, position, beam_score, k_cache, v_cache, w_query, w_key, w_value, w_out,
                   w_gate, w_up, w_down, g_attn, g_mlp, g_final, w_vocab):
        n_layers, nb, slots, heads, hd = k_cache.shape
        width = parent.shape[1]
        span = width // nb
        dm = tok_emb.shape[1]
        ff = w_gate.shape[2]
        vocab = w_vocab.shape[1]
        rows = CORES * nb
        hrow = heads * hd
        kt = k_cache.transpose(0, 1, 3, 4, 2).reshape(n_layers, nb, hrow, slots)
        vt = v_cache.transpose(0, 1, 3, 4, 2).reshape(n_layers, nb, hrow, slots)
        smem = pl.BlockSpec(memory_space=pltpu.SMEM)
        vmem = pl.BlockSpec(memory_space=pltpu.VMEM)
        hbm = pl.BlockSpec(memory_space=pl.ANY)
        sds = jax.ShapeDtypeStruct

        levels = [n for n in LEVELS if n < rows] + [rows]
        n_chips = mesh.shape['beam'] // CORES
        detour = parent.shape[0] == 2 and span == 2 * CORES and n_chips == 4
        plan, branch, pay, pm = pl.pallas_call(
            functools.partial(plan_kernel, (nb, span), levels, detour),
            out_shape=(sds((64,), jnp.int32), sds((1,), jnp.int32), sds((8, dm), F32), sds((8 * span, slots), jnp.int32)),
            in_specs=[smem, smem, vmem], out_specs=(smem, smem, vmem, vmem),
            scratch_shapes=[pltpu.SMEM((rows,), jnp.int32)],
            name='plan',
        )(parent, beam_score, tok_emb)

        half_dim = hd // 2
        lane = lax.broadcasted_iota(jnp.int32, (1, hrow), 1)
        inv_freq = ROPE_BASE ** (-2.0 * (lane % half_dim).astype(F32) / hd)
        angles = position[0].astype(F32) * inv_freq
        cos_t = jnp.cos(angles)
        sin_t = jnp.where(lane % hd < half_dim, -1.0, 1.0) * jnp.sin(angles)

        def main(n_slots, cid, *ops):
            np_ = dm // 128
            nrow = 8 * span
            dma = pltpu.SemaphoreType.DMA
            n_vbuf = VBUF if 2 * n_slots <= rows else VBUF // 2
            sizes = [hrow // of * n for _, _, n, of in SPLIT]
            nch = len(sizes)
            scratch = [
                [pltpu.VMEM((rows, n, slots), BF16) for n in sizes],
                [pltpu.VMEM((n_slots, n, slots), BF16) for n in sizes],
                [pltpu.VMEM((n_slots, n, slots), BF16) for n in sizes],
                [pltpu.VMEM((n, slots), BF16) for n in sizes],
                [pltpu.VMEM((n, slots), BF16) for n in sizes],
                [pltpu.VMEM((n, slots), BF16) for n in sizes],
                pltpu.VMEM((8, vocab), F32), pltpu.VMEM((n_layers, 2, 8, hrow), F32),
                pltpu.VMEM((n_layers, 2, nb, hrow, slots), BF16),
                pltpu.VMEM((n_layers, dm, hrow), BF16),
                pltpu.VMEM((n_layers, dm, hrow), BF16),
                pltpu.VMEM((n_layers, dm, hrow), BF16),
                pltpu.VMEM((n_layers, hrow, dm), BF16),
                pltpu.VMEM((n_layers, dm, ff), BF16),
                pltpu.VMEM((n_layers, dm, ff), BF16),
                pltpu.VMEM((n_layers, ff, dm), BF16),
                pltpu.VMEM((n_vbuf, dm, CHUNK), BF16),
                pltpu.VMEM((span, 8, dm), F32),
                pltpu.VMEM((nrow, dm), F32),
                pltpu.VMEM((nrow, dm), F32),
                pltpu.VMEM((nrow, dm), F32),
                pltpu.VMEM((nrow, dm), F32),
                pltpu.VMEM((n_layers, np_, 2, nrow, 128), F32),
                pltpu.VMEM((n_layers, sp_n, 2, nrow, 128), F32),
                pltpu.VMEM((n_layers, nrow, 128), BF16),
                pltpu.VMEM((n_layers, span * sp_n, nrow, 128), BF16),
                pltpu.VMEM((nrow, dm), F32),
                dma((span,)), dma((span,)),
                dma((nch,)), dma((nch,)), dma((nch,)), dma((nch,)), dma((2,)), dma((2,)),
                dma((nch, n_slots)), dma((nch, n_slots)), dma((nch, n_slots + 1)), dma((nch, n_slots + 1)),
                dma((nch, n_slots + 1)), dma((nch,)), dma((nch,)), dma((nch,)), dma((nch,)), dma((2,)),
                dma((2, nch)), dma((n_layers, 7)), dma((n_vbuf,)),
                dma((n_layers, sp_n)), dma((n_layers, sp_n)),
                dma((n_layers, span * sp_n)), dma((n_layers, span * sp_n)),
            ]
            return pl.pallas_call(
                functools.partial(main_kernel, (nb, span, sp_n, hd), n_slots, detour and n_slots < rows),
                out_shape=(sds((8, vocab), F32), sds((n_layers, 2, 8, hrow), F32),
                           sds((n_layers, 2, nb, hrow, slots), BF16),
                           sds((n_layers, 2, rows, hrow, slots), BF16)),
                in_specs=[smem, smem] + [vmem] * 7 + [hbm] * 10,
                out_specs=(hbm, hbm, hbm, hbm),
                scratch_shapes=scratch,
                compiler_params=pltpu.CompilerParams(collective_id=cid, has_side_effects=True,
                                                     vmem_limit_bytes=VMEM_LIMIT),
                name=f'main{n_slots}',
            )(*ops)

        ops = (plan, position, pay, pm, cos_t, sin_t, g_attn, g_mlp, g_final, kt, vt,
               w_query, w_key, w_value, w_out, w_gate, w_up, w_down, w_vocab)
        cand8, new, sib, recv = lax.switch(
            branch[0], [functools.partial(main, n, i) for i, n in enumerate(levels)], *ops)

        ko, vo, cand = pl.pallas_call(
            functools.partial(assemble_kernel, (nb,)),
            out_shape=(sds(kt.shape, BF16), sds(vt.shape, BF16), sds((nb, vocab), F32)),
            in_specs=[smem, smem, hbm, hbm, hbm, hbm, hbm, hbm],
            out_specs=(hbm, hbm, hbm),
            scratch_shapes=[pltpu.VMEM((n_layers * 2 * nb, hrow, slots), BF16),
                            pltpu.VMEM((8, vocab), F32), pltpu.VMEM((nb, vocab), F32), pltpu.VMEM((n_layers, 2, 8, hrow), F32),
                            pltpu.SemaphoreType.DMA((n_layers * 2 * nb,)),
                            pltpu.SemaphoreType.DMA((n_layers * 2 * nb,)), pltpu.SemaphoreType.DMA((3,))],
            compiler_params=pltpu.CompilerParams(vmem_limit_bytes=VMEM_LIMIT),
            name='assemble',
        )(plan, position, new, cand8, kt, vt, sib, recv)

        def back(x):
            return x.reshape(n_layers, nb, heads, hd, slots).transpose(0, 1, 4, 2, 3)

        return back(ko), back(vo), cand

    in_specs = (row_spec, P('dp', None), rep, beam_spec, cache_spec, cache_spec) + (rep,) * 11
    return jax.shard_map(local_step, mesh=mesh, in_specs=in_specs, out_specs=(cache_spec, cache_spec, row_spec),
                         check_vma=False)
```
